16 devices in a mesh: fsdp: 16 (over z, y, x, core).
Axes of the slice: x: 2, y: 2, z: 2, core: 2. Of those that a mesh axis runs over, the one named last changes fastest.
Arguments:
- token_ids: int32 [16, 512], P('fsdp')
- grad_y: bfloat16 [16, 512, 1536], P('fsdp')
- table: bfloat16 [151936, 1536], P('fsdp')
- norm1_gain: bfloat16 [1536], P('fsdp')
- norm2_gain: bfloat16 [1536], P('fsdp')
- w_query: bfloat16 [1536, 12, 128], P('fsdp')
- w_key: bfloat16 [1536, 2, 128], P('fsdp')
- w_value: bfloat16 [1536, 2, 128], P('fsdp')
- w_out: bfloat16 [1536, 1536], P('fsdp')
- w_gate: bfloat16 [1536, 8960], P('fsdp')
- w_up: bfloat16 [1536, 8960], P('fsdp')
- w_down: bfloat16 [8960, 1536], P('fsdp')
Outputs:
- output 1: bfloat16 [16, 512, 1536], P('fsdp')
- output 2: bfloat16 [151936, 1536], P('fsdp')
- output 3: bfloat16 [1536], P('fsdp')
- output 4: bfloat16 [1536], P('fsdp')
- output 5: bfloat16 [1536, 12, 128], P('fsdp')
- output 6: bfloat16 [1536, 2, 128], P('fsdp')
- output 7: bfloat16 [1536, 2, 128], P('fsdp')
- output 8: bfloat16 [1536, 1536], P('fsdp')
- output 9: bfloat16 [1536, 8960], P('fsdp')
- output 10: bfloat16 [1536, 8960], P('fsdp')
- output 11: bfloat16 [8960, 1536], P('fsdp')
All inputs are finite; a program needn't handle non-finite values.
Results may differ from the reference program's by a relative error of at most 0.0153617.
Values are sent between devices in bfloat16 or wider.
A program may use at most 1 GiB of HBM per device.

```python
import jax
import jax.numpy as jnp
from jax import lax

VOCAB_SIZE = 151936
MODEL_DIM = 1536
Q_HEADS = 12
KV_HEADS = 2
HEAD_DIM = 128
FFN_DIM = 8960
GLOBAL_BATCH = 16
SEQ_LEN = 512

NORM_EPS = 1e-5
ROPE_THETA = 500000.0
VOCAB_BITS = (VOCAB_SIZE - 1).bit_length()
TOKENS_ALL = GLOBAL_BATCH * SEQ_LEN


def draw_ids(rng_key):
    k_level, k_rank, k_flat, k_pick, k_perm = jax.random.split(rng_key, 5)
    id_shape = (GLOBAL_BATCH, SEQ_LEN)
    levels = jax.random.randint(k_level, id_shape, 0, VOCAB_BITS + 1)
    level_span = jnp.minimum(jnp.left_shift(jnp.ones(id_shape, jnp.int32), levels), VOCAB_SIZE)
    id_ranks = jax.random.randint(k_rank, id_shape, 0, level_span)
    flat_ids = jax.random.randint(k_flat, id_shape, 0, VOCAB_SIZE)
    use_flat = jax.random.randint(k_pick, id_shape, 0, 4) == 0
    id_ranks = jnp.where(use_flat, flat_ids, id_ranks)
    row_order = jax.random.permutation(k_perm, VOCAB_SIZE)
    return jnp.take(row_order, id_ranks).astype(jnp.int32)


def normal_weight(rng_key, w_shape, fan_in):
    return (jax.random.normal(rng_key, w_shape, jnp.float32) * fan_in ** -0.5).astype(jnp.bfloat16)


def setup_inputs(seed: int = 0) -> dict:
    keys = jax.random.split(jax.random.key(seed), 12)
    attn_width = Q_HEADS * HEAD_DIM
    return {
        "token_ids": draw_ids(keys[0]),
        "grad_y": (jax.random.normal(keys[1], (GLOBAL_BATCH, SEQ_LEN, MODEL_DIM), jnp.float32) * TOKENS_ALL ** -0.5).astype(jnp.bfloat16),
        "table": jax.random.normal(keys[2], (VOCAB_SIZE, MODEL_DIM), jnp.float32).astype(jnp.bfloat16),
        "norm1_gain": jax.random.uniform(keys[3], (MODEL_DIM,), jnp.float32, 0.5, 1.5).astype(jnp.bfloat16),
        "norm2_gain": jax.random.uniform(keys[4], (MODEL_DIM,), jnp.float32, 0.5, 1.5).astype(jnp.bfloat16),
        "w_query": normal_weight(keys[5], (MODEL_DIM, Q_HEADS, HEAD_DIM), MODEL_DIM),
        "w_key": normal_weight(keys[6], (MODEL_DIM, KV_HEADS, HEAD_DIM), MODEL_DIM),
        "w_value": normal_weight(keys[7], (MODEL_DIM, KV_HEADS, HEAD_DIM), MODEL_DIM),
        "w_out": normal_weight(keys[8], (attn_width, MODEL_DIM), attn_width),
        "w_gate": normal_weight(keys[9], (MODEL_DIM, FFN_DIM), MODEL_DIM),
        "w_up": normal_weight(keys[10], (MODEL_DIM, FFN_DIM), MODEL_DIM),
        "w_down": normal_weight(keys[11], (FFN_DIM, MODEL_DIM), FFN_DIM),
    }


def rms_norm(x_f32, gain_f32):
    inv_rms = lax.rsqrt(jnp.mean(x_f32 * x_f32, axis=-1, keepdims=True) + NORM_EPS)
    return (x_f32 * inv_rms * gain_f32).astype(jnp.bfloat16)


def rotary(x_f32):
    head_dim = x_f32.shape[-1]
    half_dim = head_dim // 2
    seq_len = x_f32.shape[-3]
    inv_freq = ROPE_THETA ** (-2.0 * jnp.arange(half_dim, dtype=jnp.float32) / head_dim)
    angles = jnp.arange(seq_len, dtype=jnp.float32)[:, None] * inv_freq[None, :]
    cos_tab = jnp.cos(angles)[:, None, :]
    sin_tab = jnp.sin(angles)[:, None, :]
    lo_half = x_f32[..., :half_dim]
    hi_half = x_f32[..., half_dim:]
    return jnp.concatenate([lo_half * cos_tab - hi_half * sin_tab, hi_half * cos_tab + lo_half * sin_tab], axis=-1)


def attend(q_f32, k_f32, v_bf16):
    q_rot = rotary(q_f32).astype(jnp.bfloat16).reshape(SEQ_LEN, KV_HEADS, Q_HEADS // KV_HEADS, HEAD_DIM)
    k_rot = rotary(k_f32).astype(jnp.bfloat16)
    scores = jnp.einsum("qkgd,skd->kgqs", q_rot.astype(jnp.float32), k_rot.astype(jnp.float32)) * HEAD_DIM ** -0.5
    positions = jnp.arange(SEQ_LEN)
    causal = positions[:, None] >= positions[None, :]
    scores = jnp.where(causal, scores, -1e30)
    prob_bf = jax.nn.softmax(scores, axis=-1).astype(jnp.bfloat16)
    attn_out = jnp.einsum("kgqs,skd->qkgd", prob_bf.astype(jnp.float32), v_bf16.astype(jnp.float32))
    return attn_out.astype(jnp.bfloat16).reshape(SEQ_LEN, Q_HEADS * HEAD_DIM)


def layer(emb_rows, gain_one, gain_two, w_query, w_key, w_value, w_out, w_gate, w_up, w_down):
    x_f32 = emb_rows.astype(jnp.float32)
    h_one = rms_norm(x_f32, gain_one).astype(jnp.float32)
    q_f32 = jnp.einsum("sd,dhe->she", h_one, w_query)
    k_f32 = jnp.einsum("sd,dhe->she", h_one, w_key)
    v_bf16 = jnp.einsum("sd,dhe->she", h_one, w_value).astype(jnp.bfloat16)
    attn_out = attend(q_f32, k_f32, v_bf16)
    resid_f32 = x_f32 + jnp.dot(attn_out.astype(jnp.float32), w_out, preferred_element_type=jnp.float32)
    resid_two = resid_f32.astype(jnp.bfloat16).astype(jnp.float32)
    h_two = rms_norm(resid_two, gain_two).astype(jnp.float32)
    gate_f32 = jnp.dot(h_two, w_gate, preferred_element_type=jnp.float32)
    up_f32 = jnp.dot(h_two, w_up, preferred_element_type=jnp.float32)
    act_f32 = (jax.nn.silu(gate_f32) * up_f32).astype(jnp.bfloat16).astype(jnp.float32)
    return (resid_two + jnp.dot(act_f32, w_down, preferred_element_type=jnp.float32)).astype(jnp.bfloat16)


def reference(token_ids, grad_y, table, norm1_gain, norm2_gain, w_query, w_key, w_value, w_out, w_gate, w_up, w_down):
    params = tuple(weight.astype(jnp.float32) for weight in (norm1_gain, norm2_gain, w_query, w_key, w_value, w_out, w_gate, w_up, w_down))

    def one_sequence(grad_acc, seq_in):
        seq_ids, seq_dy = seq_in
        emb_rows = jnp.take(table, seq_ids, axis=0)
        layer_out, pullback = jax.vjp(layer, emb_rows, *params)
        cotangents = pullback(seq_dy)
        new_acc = tuple(acc_old + cot_new for acc_old, cot_new in zip(grad_acc, cotangents[1:]))
        return new_acc, (layer_out, cotangents[0])

    zero_acc = tuple(jnp.zeros_like(weight) for weight in params)
    grad_acc, (y_out, d_emb) = lax.scan(one_sequence, zero_acc, (token_ids, grad_y))
    grad_table = jax.ops.segment_sum(d_emb.reshape(-1, MODEL_DIM).astype(jnp.float32), token_ids.reshape(-1), num_segments=VOCAB_SIZE).astype(jnp.bfloat16)
    grads = [acc_val.astype(jnp.bfloat16) for acc_val in grad_acc]
    return (y_out, grad_table, grads[0], grads[1], grads[2], grads[3], grads[4], grads[5], grads[6], grads[7], grads[8])
```

```python
import jax
import jax.numpy as jnp
from jax import lax
from jax.experimental import pallas as pl
from jax.experimental.pallas import tpu as pltpu
from jax.sharding import PartitionSpec as P


ALL = ("z", "y", "x", "c")
PLANE = ("z", "y")
N_DEV = 16
NORM_EPS = 1e-5
ROPE_THETA = 500000.0
SLOTS = 48
ROW_BLOCK = 128
F32 = jnp.float32
BF16 = jnp.bfloat16


def rms_norm(x_f32, gain_f32):
    inv_rms = lax.rsqrt(jnp.mean(x_f32 * x_f32, axis=-1, keepdims=True) + NORM_EPS)
    return (x_f32 * inv_rms * gain_f32).astype(BF16)


def rotary(x_f32):
    head_dim = x_f32.shape[-1]
    half_dim = head_dim // 2
    seq_len = x_f32.shape[-3]
    inv_freq = ROPE_THETA ** (-2.0 * jnp.arange(half_dim, dtype=F32) / head_dim)
    angles = jnp.arange(seq_len, dtype=F32)[:, None] * inv_freq[None, :]
    cos_tab = jnp.cos(angles)[:, None, :]
    sin_tab = jnp.sin(angles)[:, None, :]
    lo_half = x_f32[..., :half_dim]
    hi_half = x_f32[..., half_dim:]
    return jnp.concatenate([lo_half * cos_tab - hi_half * sin_tab, hi_half * cos_tab + lo_half * sin_tab], axis=-1)


def attend(q_f32, k_f32, v_bf16):
    batch_loc, seq_len, q_heads, head_dim = q_f32.shape
    kv_heads = k_f32.shape[2]
    q_rot = rotary(q_f32).astype(BF16).reshape(batch_loc, seq_len, kv_heads, q_heads // kv_heads, head_dim)
    k_rot = rotary(k_f32).astype(BF16)
    scores = jnp.einsum("bqkgd,bskd->bkgqs", q_rot, k_rot, preferred_element_type=F32) * head_dim ** -0.5
    positions = jnp.arange(seq_len)
    causal = positions[:, None] >= positions[None, :]
    scores = jnp.where(causal, scores, -1e30)
    prob_bf = jax.nn.softmax(scores, axis=-1).astype(BF16)
    attn_out = jnp.einsum("bkgqs,bskd->bqkgd", prob_bf, v_bf16, preferred_element_type=F32)
    return attn_out.astype(BF16).reshape(batch_loc, seq_len, q_heads * head_dim)


def gated(gate_f32, up_f32):
    return (jax.nn.silu(gate_f32) * up_f32).astype(BF16)


def dot(a, b, ca, cb):
    return lax.dot_general(a, b, (((ca,), (cb,)), ((), ())), preferred_element_type=F32)


def flip(a, axis):
    return lax.ppermute(a, axis, [(0, 1), (1, 0)])


def row_sum_kernel(start_ref, slot_ref, row_ref, recv_ref, out_ref, acc):
    blk = pl.program_id(0)
    acc[...] = jnp.zeros_like(acc)

    def add_row(i, carry):
        r = row_ref[i] - blk * ROW_BLOCK
        acc[pl.ds(r, 1), :] += recv_ref[pl.ds(slot_ref[i], 1), :]
        return carry

    lax.fori_loop(start_ref[blk], start_ref[blk + 1], add_row, 0)
    out_ref[...] = acc[...].astype(BF16)


def row_sums(starts, slots, rows, recv, rows_dev):
    width = recv.shape[1]
    n_blk = pl.cdiv(rows_dev, ROW_BLOCK)
    return pl.pallas_call(
        row_sum_kernel,
        out_shape=jax.ShapeDtypeStruct((rows_dev, width), BF16),
        grid_spec=pltpu.PrefetchScalarGridSpec(
            num_scalar_prefetch=3,
            grid=(n_blk,),
            in_specs=[pl.BlockSpec(recv.shape, lambda i, *_: (0, 0))],
            out_specs=pl.BlockSpec((ROW_BLOCK, width), lambda i, *_: (i, 0)),
            scratch_shapes=[pltpu.VMEM((ROW_BLOCK, width), F32)],
        ),
        compiler_params=pltpu.CompilerParams(dimension_semantics=("arbitrary",)),
        cost_estimate=pl.CostEstimate(flops=40_000_000_000, bytes_accessed=40_000_000, transcendentals=0),
    )(starts, slots, rows, recv)


def place_xc(pieces, x_i, c_i, shape, at):
    buf = jnp.zeros(shape, pieces[0].dtype)
    for k, piece in enumerate(pieces):
        px = x_i if k < 2 else 1 - x_i
        pc = c_i if k % 2 == 0 else 1 - c_i
        buf = lax.dynamic_update_slice(buf, piece, at(px, pc))
    return buf


def gather_xc(w):
    wx = flip(w, "x")
    return [w, flip(w, "c"), wx, flip(wx, "c")]


def solution(mesh):
    mesh = jax.sharding.Mesh(mesh.devices.reshape(2, 2, 2, 2), ALL)
    spec_1d = P(ALL)
    spec_2d = P(ALL, None)
    spec_3d = P(ALL, None, None)
    in_specs = (spec_2d, spec_3d, spec_2d, spec_1d, spec_1d, spec_3d, spec_3d, spec_3d, spec_2d, spec_2d, spec_2d, spec_2d)
    out_specs = (spec_3d, spec_2d, spec_1d, spec_1d, spec_3d, spec_3d, spec_3d, spec_2d, spec_2d, spec_2d, spec_2d)

    def step(token_ids, grad_y, table, gain1, gain2, w_query, w_key, w_value, w_out, w_gate, w_up, w_down):
        seq = token_ids.shape[1]
        rows_dev, dim = table.shape
        shard = w_gate.shape[0]
        ffn = w_gate.shape[1]
        ffn_q = ffn // 4
        q_w = w_query.shape[1] * w_query.shape[2]
        kv_w = w_key.shape[1] * w_key.shape[2]
        qkv_w = q_w + 2 * kv_w
        me = lax.axis_index(ALL)
        x_i, c_i = lax.axis_index("x"), lax.axis_index("c")

        small = jnp.concatenate([token_ids.astype(F32), gain1.astype(F32)[None], gain2.astype(F32)[None]], axis=1)
        small = lax.all_gather(small, ALL, axis=0, tiled=True)
        ids_all = small[:, :seq].astype(jnp.int32)
        g1_full = small[:, seq : seq + shard].reshape(-1)
        g2_full = small[:, seq + shard :].reshape(-1)

        owner = ids_all // rows_dev
        pos = jnp.arange(seq)
        before = pos[None, :] < pos[:, None]
        same = ids_all[:, :, None] == ids_all[:, None, :]
        first = jnp.logical_not(jnp.any(same & before[None], axis=2))
        mine = first & (owner == me)
        owner_is = (owner[:, :, None] == jnp.arange(N_DEV)) & first[:, :, None]
        overflow = jnp.max(jnp.sum(owner_is.astype(jnp.int32), axis=1)) > SLOTS
        rank = jnp.einsum("bt,st->bs", mine.astype(BF16), before.astype(BF16), preferred_element_type=F32).astype(jnp.int32)
        in_slot = mine[:, None, :] & (rank[:, None, :] == jnp.arange(SLOTS)[None, :, None])
        rel = ids_all - me * rows_dev
        slot_row = jnp.sum(jnp.where(in_slot, rel[:, None, :], 0), axis=2)
        slot_used = jnp.any(in_slot, axis=2)
        ids_me = token_ids[0]
        own_me = ids_me // rows_dev
        same_me = ids_me[:, None] == ids_me[None, :]
        first_me = jnp.logical_not(jnp.any(same_me & before, axis=1))
        rank_me = jnp.sum(((own_me[:, None] == own_me[None, :]) & before & first_me[None, :]).astype(jnp.int32), axis=1)
        slot_first = own_me * SLOTS + rank_me
        slot_tok = jnp.sum(jnp.where(same_me & first_me[None, :], slot_first[None, :], 0), axis=1)
        pick = (slot_tok[:, None] == jnp.arange(N_DEV * SLOTS)[None, :]).astype(BF16)

        sent = jnp.take(table, slot_row.reshape(-1), axis=0).reshape(N_DEV, SLOTS, dim)
        got = lax.all_to_all(sent, ALL, 0, 0, tiled=True)
        emb_fast = dot(pick, got.reshape(-1, dim), 1, 0).astype(BF16)

        def emb_dense():
            owned = owner == me
            picked = jnp.take(table, jnp.where(owned, rel, 0), axis=0)
            part = lax.all_to_all(jnp.where(owned[:, :, None], picked, jnp.zeros((), BF16)), ALL, 0, 0, tiled=True)
            return jnp.sum(part.astype(F32), axis=0).astype(BF16)

        emb = lax.cond(overflow, emb_dense, lambda: emb_fast)

        attn_w = jnp.concatenate([w_query.reshape(shard, -1), w_key.reshape(shard, -1), w_value.reshape(shard, -1), w_out], axis=1)
        attn_w = lax.all_gather(attn_w, ALL, axis=0, tiled=True)
        w_qkv, w_o = attn_w[:, :qkv_w], attn_w[:, qkv_w:]
        dy = grad_y[0]
        dy_all = lax.all_gather(dy, PLANE, axis=0, tiled=True)
        cols = jnp.stack([w_gate, w_up]).reshape(2, shard, 4, ffn_q).transpose(2, 0, 1, 3)
        cols = lax.all_to_all(cols, PLANE, 0, 0, tiled=True)
        wide = []
        for k in range(2):
            pieces = [p[:, None] for p in gather_xc(cols[:, k])]
            buf = place_xc([p[:, :, None] for p in pieces], x_i, c_i, (4, 2, 2, shard, ffn_q), lambda px, pc: (0, px, pc, 0, 0))
            wide.append(buf.reshape(dim, ffn_q))
        w_g, w_u = wide
        w_d = place_xc([p[None, None] for p in gather_xc(w_down)], x_i, c_i, (2, 2) + w_down.shape, lambda px, pc: (px, pc, 0, 0)).reshape(ffn_q, dim)

        x_f32 = emb.astype(F32)
        h_one, norm1_pull = jax.vjp(rms_norm, x_f32, g1_full)
        qkv = dot(h_one, w_qkv, 1, 0)
        q_f32 = qkv[:, :q_w].reshape(1, seq, -1, 128)
        k_f32 = qkv[:, q_w : q_w + kv_w].reshape(1, seq, -1, 128)
        v_bf16 = qkv[:, q_w + kv_w :].astype(BF16).reshape(1, seq, -1, 128)
        attn_out, attn_pull = jax.vjp(attend, q_f32, k_f32, v_bf16)
        o_bf = attn_out[0]
        resid_bf = (x_f32 + dot(o_bf, w_o, 1, 0)).astype(BF16)
        resid_two = resid_bf.astype(F32)
        h_two, norm2_pull = jax.vjp(rms_norm, resid_two, g2_full)

        h_all = lax.all_gather(h_two, PLANE, axis=0, tiled=True)
        d_act = dot(dy_all, w_d, 1, 1).astype(BF16)
        gate_f32 = dot(h_all, w_g, 1, 0)
        up_f32 = dot(h_all, w_u, 1, 0)
        act, act_pull = jax.vjp(gated, gate_f32, up_f32)
        d_gate, d_up = act_pull(d_act)
        d_gate, d_up = d_gate.astype(BF16), d_up.astype(BF16)
        d_h_part = dot(d_gate, w_g, 1, 1) + dot(d_up, w_u, 1, 1)
        d_h_two = lax.psum_scatter(d_h_part, PLANE, scatter_dimension=0, tiled=True).astype(BF16)
        y_part = dot(act, w_d, 1, 0)
        y_sum = lax.psum_scatter(y_part, PLANE, scatter_dimension=0, tiled=True)
        y_sum, resid_y = lax.optimization_barrier((y_sum, resid_bf))
        layer_out = (resid_y.astype(F32) + y_sum).astype(BF16)

        def reduce_xc(part, c_dim, x_dim):
            keep = lax.dynamic_index_in_dim(part, c_i, c_dim, keepdims=False)
            give = lax.dynamic_index_in_dim(part, 1 - c_i, c_dim, keepdims=False)
            got_c = flip(give, "c")
            half = keep + got_c
            keep = lax.dynamic_index_in_dim(half, x_i, x_dim, keepdims=False)
            give = lax.dynamic_index_in_dim(half, 1 - x_i, x_dim, keepdims=False)
            got_x = flip(give, "x")
            return (keep + got_x).astype(BF16)

        g_gate = dot(h_all, d_gate, 0, 0)
        g_up = dot(h_all, d_up, 0, 0)
        g_down = dot(act, dy_all, 0, 0)
        g_gate = reduce_xc(g_gate.reshape(4, 2, 2, shard, ffn_q), 2, 1)
        g_up = reduce_xc(g_up.reshape(4, 2, 2, shard, ffn_q), 2, 1)
        g_down = reduce_xc(g_down.reshape(2, 2, ffn // N_DEV, dim), 1, 0)
        back = lax.all_to_all(jnp.stack([g_gate, g_up], axis=1), PLANE, 0, 0, tiled=True)
        back = back.transpose(1, 2, 0, 3).reshape(2, shard, ffn)

        d_resid_two, g_norm2 = norm2_pull(d_h_two)
        d_resid = (dy.astype(F32) + d_resid_two).astype(BF16)
        g_out = dot(o_bf, d_resid, 0, 0)
        g_out = lax.psum_scatter(g_out, ALL, scatter_dimension=0, tiled=True).astype(BF16)
        d_attn = dot(d_resid, w_o, 1, 1).astype(BF16)
        d_query, d_key, d_value = attn_pull(d_attn[None])
        d_qkv = jnp.concatenate([d_query.astype(BF16).reshape(seq, -1), d_key.astype(BF16).reshape(seq, -1), d_value.reshape(seq, -1)], axis=1)
        g_qkv = dot(h_one, d_qkv, 0, 0)
        g_qkv = lax.psum_scatter(g_qkv, ALL, scatter_dimension=0, tiled=True).astype(BF16)
        d_h_one = dot(d_qkv, w_qkv, 1, 1).astype(BF16)
        d_x, g_norm1 = norm1_pull(d_h_one)
        d_emb = (d_resid.astype(F32) + d_x).astype(BF16)

        d_slot = dot(pick, d_emb, 0, 0).reshape(N_DEV, SLOTS, dim)
        extra = jnp.broadcast_to(jnp.concatenate([g_norm1[None], g_norm2[None], jnp.zeros((6, dim), F32)])[None], (N_DEV, 8, dim))
        d_got = lax.all_to_all(jnp.concatenate([d_slot, extra], axis=1), ALL, 0, 0, tiled=True)
        gains = lax.dynamic_slice_in_dim(jnp.sum(d_got[:, SLOTS : SLOTS + 2], axis=0), me * shard, shard, axis=1).astype(BF16)
        stride = SLOTS + 8
        n_slot = N_DEV * stride
        key = jnp.pad(jnp.where(slot_used, slot_row, rows_dev), ((0, 0), (0, 8)), constant_values=rows_dev).reshape(-1)
        key_sorted, order = lax.sort((key, jnp.arange(n_slot, dtype=jnp.int32)), num_keys=1)
        edges = jnp.minimum(jnp.arange(pl.cdiv(rows_dev, ROW_BLOCK) + 1) * ROW_BLOCK, rows_dev)
        starts = jnp.sum((key[None, :] < edges[:, None]).astype(jnp.int32), axis=1)

        def rows_dense():
            d_all = lax.all_to_all(jnp.broadcast_to(d_emb[None], (N_DEV, seq, dim)), ALL, 0, 0, tiled=True).reshape(-1, dim)
            seg = jnp.where(owner == me, rel, rows_dev).reshape(-1)
            return jax.ops.segment_sum(d_all.astype(F32), seg, num_segments=rows_dev).astype(BF16)

        d_rows = lax.cond(overflow, rows_dense, lambda: row_sums(starts, order, key_sorted, d_got.reshape(-1, dim), rows_dev))
        g_q = g_qkv[:, :q_w].reshape(w_query.shape)
        g_k = g_qkv[:, q_w : q_w + kv_w].reshape(w_key.shape)
        g_v = g_qkv[:, q_w + kv_w :].reshape(w_value.shape)
        return layer_out[None], d_rows, gains[0], gains[1], g_q, g_k, g_v, g_out, back[0], back[1], g_down


    return jax.shard_map(step, mesh=mesh, in_specs=in_specs, out_specs=out_specs, check_vma=False)
```

```python
import jax
import jax.numpy as jnp
from jax import lax
from jax.experimental import pallas as pl
from jax.experimental.pallas import tpu as pltpu
from jax.sharding import PartitionSpec as P


ALL = ("z", "y", "x", "c")
PLANE = ("z", "y")
N_DEV = 16
NORM_EPS = 1e-5
ROPE_THETA = 500000.0
SLOTS = 48
USABLE = SLOTS - 2
ROW_BLOCK = 128
F32 = jnp.float32
BF16 = jnp.bfloat16


def rms_norm(x_f32, gain_f32):
    inv_rms = lax.rsqrt(jnp.mean(x_f32 * x_f32, axis=-1, keepdims=True) + NORM_EPS)
    return (x_f32 * inv_rms * gain_f32).astype(BF16)


def rotary(x_f32):
    head_dim = x_f32.shape[-1]
    half_dim = head_dim // 2
    seq_len = x_f32.shape[-3]
    inv_freq = ROPE_THETA ** (-2.0 * jnp.arange(half_dim, dtype=F32) / head_dim)
    angles = jnp.arange(seq_len, dtype=F32)[:, None] * inv_freq[None, :]
    cos_tab = jnp.cos(angles)[:, None, :]
    sin_tab = jnp.sin(angles)[:, None, :]
    lo_half = x_f32[..., :half_dim]
    hi_half = x_f32[..., half_dim:]
    return jnp.concatenate([lo_half * cos_tab - hi_half * sin_tab, hi_half * cos_tab + lo_half * sin_tab], axis=-1)


def attend(q_f32, k_f32, v_bf16):
    batch_loc, seq_len, q_heads, head_dim = q_f32.shape
    kv_heads = k_f32.shape[2]
    q_rot = rotary(q_f32).astype(BF16).reshape(batch_loc, seq_len, kv_heads, q_heads // kv_heads, head_dim)
    k_rot = rotary(k_f32).astype(BF16)
    scores = jnp.einsum("bqkgd,bskd->bkgqs", q_rot, k_rot, preferred_element_type=F32) * head_dim ** -0.5
    positions = jnp.arange(seq_len)
    causal = positions[:, None] >= positions[None, :]
    scores = jnp.where(causal, scores, -1e30)
    prob_bf = jax.nn.softmax(scores, axis=-1).astype(BF16)
    attn_out = jnp.einsum("bkgqs,bskd->bqkgd", prob_bf, v_bf16, preferred_element_type=F32)
    return attn_out.astype(BF16).reshape(batch_loc, seq_len, q_heads * head_dim)


def gated(gate_f32, up_f32):
    return (jax.nn.silu(gate_f32) * up_f32).astype(BF16)


def dot(a, b, ca, cb):
    return lax.dot_general(a, b, (((ca,), (cb,)), ((), ())), preferred_element_type=F32)


def flip(a, axis):
    return lax.ppermute(a, axis, [(0, 1), (1, 0)])


def row_sum_kernel(start_ref, slot_ref, row_ref, recv_ref, out_ref, acc):
    blk = pl.program_id(0)
    acc[...] = jnp.zeros_like(acc)

    def add_row(i, carry):
        r = row_ref[i] - blk * ROW_BLOCK
        acc[pl.ds(r, 1), :] += recv_ref[pl.ds(slot_ref[i], 1), :]
        return carry

    lax.fori_loop(start_ref[blk], start_ref[blk + 1], add_row, 0)
    out_ref[...] = acc[...].astype(BF16)


def row_sums(starts, slots, rows, recv, rows_dev):
    width = recv.shape[1]
    n_blk = pl.cdiv(rows_dev, ROW_BLOCK)
    return pl.pallas_call(
        row_sum_kernel,
        out_shape=jax.ShapeDtypeStruct((rows_dev, width), BF16),
        grid_spec=pltpu.PrefetchScalarGridSpec(
            num_scalar_prefetch=3,
            grid=(n_blk,),
            in_specs=[pl.BlockSpec(recv.shape, lambda i, *_: (0, 0))],
            out_specs=pl.BlockSpec((ROW_BLOCK, width), lambda i, *_: (i, 0)),
            scratch_shapes=[pltpu.VMEM((ROW_BLOCK, width), F32)],
        ),
        compiler_params=pltpu.CompilerParams(dimension_semantics=("arbitrary",)),
        cost_estimate=pl.CostEstimate(flops=40_000_000_000, bytes_accessed=40_000_000, transcendentals=0),
    )(starts, slots, rows, recv)


def place_xc(pieces, x_i, c_i, shape, at):
    buf = jnp.zeros(shape, pieces[0].dtype)
    for k, piece in enumerate(pieces):
        px = x_i if k < 2 else 1 - x_i
        pc = c_i if k % 2 == 0 else 1 - c_i
        buf = lax.dynamic_update_slice(buf, piece, at(px, pc))
    return buf


def solution(mesh):
    mesh = jax.sharding.Mesh(mesh.devices.reshape(2, 2, 2, 2), ALL)
    spec_1d = P(ALL)
    spec_2d = P(ALL, None)
    spec_3d = P(ALL, None, None)
    in_specs = (spec_2d, spec_3d, spec_2d, spec_1d, spec_1d, spec_3d, spec_3d, spec_3d, spec_2d, spec_2d, spec_2d, spec_2d)
    out_specs = (spec_3d, spec_2d, spec_1d, spec_1d, spec_3d, spec_3d, spec_3d, spec_2d, spec_2d, spec_2d, spec_2d)

    def step(token_ids, grad_y, table, gain1, gain2, w_query, w_key, w_value, w_out, w_gate, w_up, w_down):
        seq = token_ids.shape[1]
        rows_dev, dim = table.shape
        shard = w_gate.shape[0]
        ffn = w_gate.shape[1]
        ffn_q = ffn // 4
        q_w = w_query.shape[1] * w_query.shape[2]
        kv_w = w_key.shape[1] * w_key.shape[2]
        qkv_w = q_w + 2 * kv_w
        me = lax.axis_index(ALL)
        x_i, c_i = lax.axis_index("x"), lax.axis_index("c")

        small = jnp.concatenate([token_ids.astype(F32), gain1.astype(F32)[None], gain2.astype(F32)[None]], axis=1)
        small = lax.all_gather(small, ALL, axis=0, tiled=True)
        ids_all = small[:, :seq].astype(jnp.int32)
        g1_full = small[:, seq : seq + shard].reshape(-1)
        g2_full = small[:, seq + shard :].reshape(-1)

        owner = ids_all // rows_dev
        pos = jnp.arange(seq)
        before = pos[None, :] < pos[:, None]
        same = ids_all[:, :, None] == ids_all[:, None, :]
        first = jnp.logical_not(jnp.any(same & before[None], axis=2))
        mine = first & (owner == me)
        owner_is = (owner[:, :, None] == jnp.arange(N_DEV)) & first[:, :, None]
        overflow = jnp.max(jnp.sum(owner_is.astype(jnp.int32), axis=1)) > USABLE
        rank = jnp.einsum("bt,st->bs", mine.astype(BF16), before.astype(BF16), preferred_element_type=F32).astype(jnp.int32)
        in_slot = mine[:, None, :] & (rank[:, None, :] == jnp.arange(SLOTS)[None, :, None])
        rel = ids_all - me * rows_dev
        slot_row = jnp.sum(jnp.where(in_slot, rel[:, None, :], 0), axis=2)
        slot_used = jnp.any(in_slot, axis=2)
        spread = (jnp.arange(N_DEV * SLOTS).reshape(N_DEV, SLOTS) * 12) % rows_dev
        fetch_row = jnp.where(slot_used, slot_row, spread)
        ids_me = token_ids[0]
        own_me = ids_me // rows_dev
        same_me = ids_me[:, None] == ids_me[None, :]
        first_me = jnp.logical_not(jnp.any(same_me & before, axis=1))
        rank_me = jnp.sum(((own_me[:, None] == own_me[None, :]) & before & first_me[None, :]).astype(jnp.int32), axis=1)
        slot_first = own_me * SLOTS + rank_me
        slot_tok = jnp.sum(jnp.where(same_me & first_me[None, :], slot_first[None, :], 0), axis=1)
        pick = (slot_tok[:, None] == jnp.arange(N_DEV * SLOTS)[None, :]).astype(BF16)

        sent = table.at[fetch_row.reshape(-1)].get(mode="promise_in_bounds").reshape(N_DEV, SLOTS, dim)
        got = lax.all_to_all(sent, ALL, 0, 0, tiled=True)
        emb_fast = dot(pick, got.reshape(-1, dim), 1, 0).astype(BF16)

        def emb_dense():
            owned = owner == me
            picked = jnp.take(table, jnp.where(owned, rel, 0), axis=0)
            part = jnp.where(owned[:, :, None], picked, jnp.zeros((), BF16))
            total = lax.dynamic_index_in_dim(part, me, 0, keepdims=False)
            for k in range(1, N_DEV):
                out = lax.dynamic_index_in_dim(part, (me + k) % N_DEV, 0, keepdims=False)
                total += lax.ppermute(out, ALL, [(d, (d + k) % N_DEV) for d in range(N_DEV)])
            return total

        emb = lax.cond(overflow, emb_dense, lambda: emb_fast)

        attn_w = jnp.concatenate([w_query.reshape(shard, -1), w_key.reshape(shard, -1), w_value.reshape(shard, -1), w_out], axis=1)
        attn_w = lax.all_gather(attn_w, ALL, axis=0, tiled=True)
        w_qkv, w_o = attn_w[:, :qkv_w], attn_w[:, qkv_w:]
        dy = grad_y[0]
        dy_all = lax.all_gather(dy, PLANE, axis=0, tiled=True)

        def gather_xc(w):
            wx = flip(w, "x")
            return [w, flip(w, "c"), wx, flip(wx, "c")]

        def wide(w):
            cols = jnp.stack([w[:, k * ffn_q : (k + 1) * ffn_q] for k in range(4)])
            cols = lax.all_to_all(cols, PLANE, 0, 0, tiled=True)
            pieces = [p[:, None, None] for p in gather_xc(cols)]
            return place_xc(pieces, x_i, c_i, (4, 2, 2, shard, ffn_q), lambda px, pc: (0, px, pc, 0, 0)).reshape(dim, ffn_q)

        w_d = place_xc([p[None, None] for p in gather_xc(w_down)], x_i, c_i, (2, 2) + w_down.shape, lambda px, pc: (px, pc, 0, 0)).reshape(ffn_q, dim)
        w_g = wide(w_gate)
        w_u = wide(w_up)

        x_f32 = emb.astype(F32)
        h_one, norm1_pull = jax.vjp(rms_norm, x_f32, g1_full)
        qkv = dot(h_one, w_qkv, 1, 0)
        q_f32 = qkv[:, :q_w].reshape(1, seq, -1, 128)
        k_f32 = qkv[:, q_w : q_w + kv_w].reshape(1, seq, -1, 128)
        v_bf16 = qkv[:, q_w + kv_w :].astype(BF16).reshape(1, seq, -1, 128)
        attn_out, attn_pull = jax.vjp(attend, q_f32, k_f32, v_bf16)
        o_bf = attn_out[0]
        resid_bf = (x_f32 + dot(o_bf, w_o, 1, 0)).astype(BF16)
        resid_two = resid_bf.astype(F32)
        h_two, norm2_pull = jax.vjp(rms_norm, resid_two, g2_full)

        h_all = lax.all_gather(h_two, PLANE, axis=0, tiled=True)
        d_act = dot(dy_all, w_d, 1, 1).astype(BF16)
        gate_f32 = dot(h_all, w_g, 1, 0)
        up_f32 = dot(h_all, w_u, 1, 0)
        act, act_pull = jax.vjp(gated, gate_f32, up_f32)
        d_gate, d_up = act_pull(d_act)
        d_gate, d_up = d_gate.astype(BF16), d_up.astype(BF16)
        d_h_part = dot(d_gate, w_g, 1, 1) + dot(d_up, w_u, 1, 1)
        d_h_two = lax.psum_scatter(d_h_part, PLANE, scatter_dimension=0, tiled=True).astype(BF16)
        y_part = dot(act, w_d, 1, 0)
        y_sum = lax.psum_scatter(y_part, PLANE, scatter_dimension=0, tiled=True)
        y_sum, resid_y = lax.optimization_barrier((y_sum, resid_bf))
        layer_out = (resid_y.astype(F32) + y_sum).astype(BF16)

        def reduce_xc(part, c_dim, x_dim):
            keep = lax.dynamic_index_in_dim(part, c_i, c_dim, keepdims=False)
            give = lax.dynamic_index_in_dim(part, 1 - c_i, c_dim, keepdims=False)
            got_c = flip(give, "c")
            half = keep + got_c
            keep = lax.dynamic_index_in_dim(half, x_i, x_dim, keepdims=False)
            give = lax.dynamic_index_in_dim(half, 1 - x_i, x_dim, keepdims=False)
            got_x = flip(give, "x")
            return (keep + got_x).astype(BF16)

        g_gate = dot(h_all, d_gate, 0, 0)
        g_up = dot(h_all, d_up, 0, 0)
        g_down = dot(act, dy_all, 0, 0)
        g_gate = reduce_xc(g_gate.reshape(4, 2, 2, shard, ffn_q), 2, 1)
        g_up = reduce_xc(g_up.reshape(4, 2, 2, shard, ffn_q), 2, 1)
        g_down = reduce_xc(g_down.reshape(2, 2, ffn // N_DEV, dim), 1, 0)
        back = lax.all_to_all(jnp.stack([g_gate, g_up], axis=1), PLANE, 0, 0, tiled=True)
        back = back.transpose(1, 2, 0, 3).reshape(2, shard, ffn)

        d_resid_two, g_norm2 = norm2_pull(d_h_two)
        d_resid = (dy.astype(F32) + d_resid_two).astype(BF16)
        g_out = dot(o_bf, d_resid, 0, 0)
        g_out = lax.psum_scatter(g_out, ALL, scatter_dimension=0, tiled=True).astype(BF16)
        d_attn = dot(d_resid, w_o, 1, 1).astype(BF16)
        d_query, d_key, d_value = attn_pull(d_attn[None])
        d_qkv = jnp.concatenate([d_query.astype(BF16).reshape(seq, -1), d_key.astype(BF16).reshape(seq, -1), d_value.reshape(seq, -1)], axis=1)
        g_qkv = dot(h_one, d_qkv, 0, 0)
        g_qkv = lax.psum_scatter(g_qkv, ALL, scatter_dimension=0, tiled=True).astype(BF16)
        d_h_one = dot(d_qkv, w_qkv, 1, 1).astype(BF16)
        d_x, g_norm1 = norm1_pull(d_h_one)
        d_emb = (d_resid.astype(F32) + d_x).astype(BF16)

        d_slot = dot(pick, d_emb, 0, 0).reshape(N_DEV, SLOTS, dim)
        place = jnp.arange(SLOTS)[None, :, None]
        d_slot = jnp.where(place == USABLE, g_norm1, jnp.where(place == USABLE + 1, g_norm2, d_slot))
        d_got = lax.all_to_all(d_slot, ALL, 0, 0, tiled=True)
        gains = lax.dynamic_slice_in_dim(jnp.sum(d_got[:, USABLE:], axis=0), me * shard, shard, axis=1).astype(BF16)
        n_slot = N_DEV * SLOTS
        key = jnp.where(slot_used, slot_row, rows_dev).reshape(-1)
        key_sorted, order = lax.sort((key, jnp.arange(n_slot, dtype=jnp.int32)), num_keys=1)
        edges = jnp.minimum(jnp.arange(pl.cdiv(rows_dev, ROW_BLOCK) + 1) * ROW_BLOCK, rows_dev)
        starts = jnp.sum((key[None, :] < edges[:, None]).astype(jnp.int32), axis=1)

        def rows_dense():
            d_all = [d_emb] + [lax.ppermute(d_emb, ALL, [(d, (d + k) % N_DEV) for d in range(N_DEV)]) for k in range(1, N_DEV)]
            d_all = jnp.concatenate(d_all, axis=0)
            origin = (me - jnp.arange(N_DEV)) % N_DEV
            seg = jnp.where(owner == me, rel, rows_dev)[origin].reshape(-1)
            return jax.ops.segment_sum(d_all.astype(F32), seg, num_segments=rows_dev).astype(BF16)

        d_rows = lax.cond(overflow, rows_dense, lambda: row_sums(starts, order, key_sorted, d_got.reshape(-1, dim), rows_dev))
        g_q = g_qkv[:, :q_w].reshape(w_query.shape)
        g_k = g_qkv[:, q_w : q_w + kv_w].reshape(w_key.shape)
        g_v = g_qkv[:, q_w + kv_w :].reshape(w_value.shape)
        return layer_out[None], d_rows, gains[0], gains[1], g_q, g_k, g_v, g_out, back[0], back[1], g_down


    return jax.shard_map(step, mesh=mesh, in_specs=in_specs, out_specs=out_specs, check_vma=False)
```

```python
import jax
import jax.numpy as jnp
from jax import lax
from jax.experimental import pallas as pl
from jax.experimental.pallas import tpu as pltpu
from jax.sharding import PartitionSpec as P


ALL = ("z", "y", "x", "c")
PLANE = ("z", "y")
N_DEV = 16
NORM_EPS = 1e-5
ROPE_THETA = 500000.0
SLOTS = 48
USABLE = SLOTS - 2
ROW_BLOCK = 128
CHUNKS = 2
F32 = jnp.float32
BF16 = jnp.bfloat16


def rms_norm(x_f32, gain_f32):
    inv_rms = lax.rsqrt(jnp.mean(x_f32 * x_f32, axis=-1, keepdims=True) + NORM_EPS)
    return (x_f32 * inv_rms * gain_f32).astype(BF16)


def rotary(x_f32):
    head_dim = x_f32.shape[-1]
    half_dim = head_dim // 2
    seq_len = x_f32.shape[-3]
    inv_freq = ROPE_THETA ** (-2.0 * jnp.arange(half_dim, dtype=F32) / head_dim)
    angles = jnp.arange(seq_len, dtype=F32)[:, None] * inv_freq[None, :]
    cos_tab = jnp.cos(angles)[:, None, :]
    sin_tab = jnp.sin(angles)[:, None, :]
    lo_half = x_f32[..., :half_dim]
    hi_half = x_f32[..., half_dim:]
    return jnp.concatenate([lo_half * cos_tab - hi_half * sin_tab, hi_half * cos_tab + lo_half * sin_tab], axis=-1)


def attend(q_f32, k_f32, v_bf16):
    batch_loc, seq_len, q_heads, head_dim = q_f32.shape
    kv_heads = k_f32.shape[2]
    q_rot = rotary(q_f32).astype(BF16).reshape(batch_loc, seq_len, kv_heads, q_heads // kv_heads, head_dim)
    k_rot = rotary(k_f32).astype(BF16)
    scores = jnp.einsum("bqkgd,bskd->bkgqs", q_rot, k_rot, preferred_element_type=F32) * head_dim ** -0.5
    positions = jnp.arange(seq_len)
    causal = positions[:, None] >= positions[None, :]
    scores = jnp.where(causal, scores, -1e30)
    prob_bf = jax.nn.softmax(scores, axis=-1).astype(BF16)
    attn_out = jnp.einsum("bkgqs,bskd->bqkgd", prob_bf, v_bf16, preferred_element_type=F32)
    return attn_out.astype(BF16).reshape(batch_loc, seq_len, q_heads * head_dim)


def gated(gate_f32, up_f32):
    return (jax.nn.silu(gate_f32) * up_f32).astype(BF16)


def dot(a, b, ca, cb):
    return lax.dot_general(a, b, (((ca,), (cb,)), ((), ())), preferred_element_type=F32)


def flip(a, axis):
    return lax.ppermute(a, axis, [(0, 1), (1, 0)])


def row_sum_kernel(start_ref, slot_ref, row_ref, recv_ref, out_ref, acc):
    blk = pl.program_id(0)
    acc[...] = jnp.zeros_like(acc)

    def add_row(i, carry):
        r = row_ref[i] - blk * ROW_BLOCK
        acc[pl.ds(r, 1), :] += recv_ref[pl.ds(slot_ref[i], 1), :]
        return carry

    lax.fori_loop(start_ref[blk], start_ref[blk + 1], add_row, 0)
    out_ref[...] = acc[...].astype(BF16)


def row_sums(starts, slots, rows, recv, rows_dev):
    width = recv.shape[1]
    n_blk = pl.cdiv(rows_dev, ROW_BLOCK)
    return pl.pallas_call(
        row_sum_kernel,
        out_shape=jax.ShapeDtypeStruct((rows_dev, width), BF16),
        grid_spec=pltpu.PrefetchScalarGridSpec(
            num_scalar_prefetch=3,
            grid=(n_blk,),
            in_specs=[pl.BlockSpec(recv.shape, lambda i, *_: (0, 0))],
            out_specs=pl.BlockSpec((ROW_BLOCK, width), lambda i, *_: (i, 0)),
            scratch_shapes=[pltpu.VMEM((ROW_BLOCK, width), F32)],
        ),
        compiler_params=pltpu.CompilerParams(dimension_semantics=("arbitrary",)),
        cost_estimate=pl.CostEstimate(flops=40_000_000_000, bytes_accessed=40_000_000, transcendentals=0),
    )(starts, slots, rows, recv)


def place_xc(pieces, x_i, c_i, shape, at):
    buf = jnp.zeros(shape, pieces[0].dtype)
    for k, piece in enumerate(pieces):
        px = x_i if k < 2 else 1 - x_i
        pc = c_i if k % 2 == 0 else 1 - c_i
        buf = lax.dynamic_update_slice(buf, piece, at(px, pc))
    return buf


def solution(mesh):
    mesh = jax.sharding.Mesh(mesh.devices.reshape(2, 2, 2, 2), ALL)
    spec_1d = P(ALL)
    spec_2d = P(ALL, None)
    spec_3d = P(ALL, None, None)
    in_specs = (spec_2d, spec_3d, spec_2d, spec_1d, spec_1d, spec_3d, spec_3d, spec_3d, spec_2d, spec_2d, spec_2d, spec_2d)
    out_specs = (spec_3d, spec_2d, spec_1d, spec_1d, spec_3d, spec_3d, spec_3d, spec_2d, spec_2d, spec_2d, spec_2d)

    def step(token_ids, grad_y, table, gain1, gain2, w_query, w_key, w_value, w_out, w_gate, w_up, w_down):
        seq = token_ids.shape[1]
        rows_dev, dim = table.shape
        shard = w_gate.shape[0]
        ffn = w_gate.shape[1]
        ffn_q = ffn // 4
        q_w = w_query.shape[1] * w_query.shape[2]
        kv_w = w_key.shape[1] * w_key.shape[2]
        qkv_w = q_w + 2 * kv_w
        me = lax.axis_index(ALL)
        x_i, c_i = lax.axis_index("x"), lax.axis_index("c")

        small = jnp.concatenate([token_ids.astype(F32), gain1.astype(F32)[None], gain2.astype(F32)[None]], axis=1)
        small = lax.all_gather(small, ALL, axis=0, tiled=True)
        ids_all = small[:, :seq].astype(jnp.int32)
        g1_full = small[:, seq : seq + shard].reshape(-1)
        g2_full = small[:, seq + shard :].reshape(-1)

        owner = ids_all // rows_dev
        pos = jnp.arange(seq)
        before = pos[None, :] < pos[:, None]
        same = ids_all[:, :, None] == ids_all[:, None, :]
        first = jnp.logical_not(jnp.any(same & before[None], axis=2))
        mine = first & (owner == me)
        owner_is = (owner[:, :, None] == jnp.arange(N_DEV)) & first[:, :, None]
        overflow = jnp.max(jnp.sum(owner_is.astype(jnp.int32), axis=1)) > USABLE
        rank = jnp.einsum("bt,st->bs", mine.astype(BF16), before.astype(BF16), preferred_element_type=F32).astype(jnp.int32)
        in_slot = mine[:, None, :] & (rank[:, None, :] == jnp.arange(SLOTS)[None, :, None])
        rel = ids_all - me * rows_dev
        slot_row = jnp.sum(jnp.where(in_slot, rel[:, None, :], 0), axis=2)
        slot_used = jnp.any(in_slot, axis=2)
        spread = (jnp.arange(N_DEV * SLOTS).reshape(N_DEV, SLOTS) * 12) % rows_dev
        fetch_row = jnp.where(slot_used, slot_row, spread)
        ids_me = token_ids[0]
        own_me = ids_me // rows_dev
        same_me = ids_me[:, None] == ids_me[None, :]
        first_me = jnp.logical_not(jnp.any(same_me & before, axis=1))
        rank_me = jnp.sum(((own_me[:, None] == own_me[None, :]) & before & first_me[None, :]).astype(jnp.int32), axis=1)
        slot_first = own_me * SLOTS + rank_me
        slot_tok = jnp.sum(jnp.where(same_me & first_me[None, :], slot_first[None, :], 0), axis=1)
        pick = (slot_tok[:, None] == jnp.arange(N_DEV * SLOTS)[None, :]).astype(BF16)

        sent = table.at[fetch_row.reshape(-1)].get(mode="promise_in_bounds").reshape(N_DEV, SLOTS, dim)
        got = lax.all_to_all(sent, ALL, 0, 0, tiled=True)
        emb_fast = dot(pick, got.reshape(-1, dim), 1, 0).astype(BF16)

        def emb_dense():
            owned = owner == me
            picked = jnp.take(table, jnp.where(owned, rel, 0), axis=0)
            part = jnp.where(owned[:, :, None], picked, jnp.zeros((), BF16))
            total = lax.dynamic_index_in_dim(part, me, 0, keepdims=False)
            for k in range(1, N_DEV):
                out = lax.dynamic_index_in_dim(part, (me + k) % N_DEV, 0, keepdims=False)
                total += lax.ppermute(out, ALL, [(d, (d + k) % N_DEV) for d in range(N_DEV)])
            return total

        emb = lax.cond(overflow, emb_dense, lambda: emb_fast)

        attn_w = jnp.concatenate([w_query.reshape(shard, -1), w_key.reshape(shard, -1), w_value.reshape(shard, -1), w_out], axis=1)
        attn_w = lax.all_gather(attn_w, ALL, axis=0, tiled=True)
        w_qkv, w_o = attn_w[:, :qkv_w], attn_w[:, qkv_w:]
        dy = grad_y[0]
        dy_all = lax.all_gather(dy, PLANE, axis=0, tiled=True)
        dy_all = dy_all.reshape(4, CHUNKS, -1, dim).transpose(1, 0, 2, 3).reshape(-1, dim)

        def gather_xc(w):
            wx = flip(w, "x")
            return [w, flip(w, "c"), wx, flip(wx, "c")]

        def wide(w):
            cols = jnp.stack([w[:, k * ffn_q : (k + 1) * ffn_q] for k in range(4)])
            cols = lax.all_to_all(cols, PLANE, 0, 0, tiled=True)
            pieces = [p[:, None, None] for p in gather_xc(cols)]
            return place_xc(pieces, x_i, c_i, (4, 2, 2, shard, ffn_q), lambda px, pc: (0, px, pc, 0, 0)).reshape(dim, ffn_q)

        w_d = place_xc([p[None, None] for p in gather_xc(w_down)], x_i, c_i, (2, 2) + w_down.shape, lambda px, pc: (px, pc, 0, 0)).reshape(ffn_q, dim)
        w_g = wide(w_gate)
        w_u = wide(w_up)

        x_f32 = emb.astype(F32)
        h_one, norm1_pull = jax.vjp(rms_norm, x_f32, g1_full)
        qkv = dot(h_one, w_qkv, 1, 0)
        q_f32 = qkv[:, :q_w].reshape(1, seq, -1, 128)
        k_f32 = qkv[:, q_w : q_w + kv_w].reshape(1, seq, -1, 128)
        v_bf16 = qkv[:, q_w + kv_w :].astype(BF16).reshape(1, seq, -1, 128)
        attn_out, attn_pull = jax.vjp(attend, q_f32, k_f32, v_bf16)
        o_bf = attn_out[0]
        resid_bf = (x_f32 + dot(o_bf, w_o, 1, 0)).astype(BF16)
        resid_two = resid_bf.astype(F32)
        h_two, norm2_pull = jax.vjp(rms_norm, resid_two, g2_full)

        step_t = seq // CHUNKS
        h_own = h_two.reshape(CHUNKS, step_t, dim)
        hs, acts, d_gates, d_ups, d_hs = [], [], [], [], []
        for k in range(CHUNKS):
            d_act = dot(lax.slice_in_dim(dy_all, k * 4 * step_t, (k + 1) * 4 * step_t), w_d, 1, 1).astype(BF16)
            h_k = lax.all_gather(h_own[k], PLANE, axis=0, tiled=True)
            gate_f32 = dot(h_k, w_g, 1, 0)
            up_f32 = dot(h_k, w_u, 1, 0)
            act_k, act_pull = jax.vjp(gated, gate_f32, up_f32)
            d_gate, d_up = act_pull(d_act)
            act_k, d_gate, d_up = lax.optimization_barrier((act_k, d_gate.astype(BF16), d_up.astype(BF16)))
            d_h_part = dot(d_gate, w_g, 1, 1) + dot(d_up, w_u, 1, 1)
            d_hs.append(lax.psum_scatter(d_h_part, PLANE, scatter_dimension=0, tiled=True).astype(BF16))
            hs.append(h_k)
            acts.append(act_k)
            d_gates.append(d_gate)
            d_ups.append(d_up)
        d_h_two = jnp.concatenate(d_hs)
        y_sums = []
        for k in range(CHUNKS):
            y_part = dot(acts[k], w_d, 1, 0)
            y_sums.append(lax.psum_scatter(y_part, PLANE, scatter_dimension=0, tiled=True))
        y_sum, resid_y = lax.optimization_barrier((jnp.concatenate(y_sums), resid_bf))
        layer_out = (resid_y.astype(F32) + y_sum).astype(BF16)
        h_all, act, d_gate, d_up = (jnp.concatenate(v) for v in (hs, acts, d_gates, d_ups))

        def reduce_xc(part, c_dim, x_dim):
            keep = lax.dynamic_index_in_dim(part, c_i, c_dim, keepdims=False)
            give = lax.dynamic_index_in_dim(part, 1 - c_i, c_dim, keepdims=False)
            got_c = flip(give, "c")
            half = keep + got_c
            keep = lax.dynamic_index_in_dim(half, x_i, x_dim, keepdims=False)
            give = lax.dynamic_index_in_dim(half, 1 - x_i, x_dim, keepdims=False)
            got_x = flip(give, "x")
            return (keep + got_x).astype(BF16)

        g_gate = dot(h_all, d_gate, 0, 0)
        g_up = dot(h_all, d_up, 0, 0)
        g_down = dot(act, dy_all, 0, 0)
        g_gate = reduce_xc(g_gate.reshape(4, 2, 2, shard, ffn_q), 2, 1)
        g_up = reduce_xc(g_up.reshape(4, 2, 2, shard, ffn_q), 2, 1)
        g_down = reduce_xc(g_down.reshape(2, 2, ffn // N_DEV, dim), 1, 0)
        back = lax.all_to_all(jnp.stack([g_gate, g_up], axis=1), PLANE, 0, 0, tiled=True)
        back = back.transpose(1, 2, 0, 3).reshape(2, shard, ffn)

        d_resid_two, g_norm2 = norm2_pull(d_h_two)
        d_resid = (dy.astype(F32) + d_resid_two).astype(BF16)
        g_out = dot(o_bf, d_resid, 0, 0)
        g_out = lax.psum_scatter(g_out, ALL, scatter_dimension=0, tiled=True).astype(BF16)
        d_attn = dot(d_resid, w_o, 1, 1).astype(BF16)
        d_query, d_key, d_value = attn_pull(d_attn[None])
        d_qkv = jnp.concatenate([d_query.astype(BF16).reshape(seq, -1), d_key.astype(BF16).reshape(seq, -1), d_value.reshape(seq, -1)], axis=1)
        g_qkv = dot(h_one, d_qkv, 0, 0)
        g_qkv = lax.psum_scatter(g_qkv, ALL, scatter_dimension=0, tiled=True).astype(BF16)
        d_h_one = dot(d_qkv, w_qkv, 1, 1).astype(BF16)
        d_x, g_norm1 = norm1_pull(d_h_one)
        d_emb = (d_resid.astype(F32) + d_x).astype(BF16)

        d_slot = dot(pick, d_emb, 0, 0).reshape(N_DEV, SLOTS, dim)
        place = jnp.arange(SLOTS)[None, :, None]
        d_slot = jnp.where(place == USABLE, g_norm1, jnp.where(place == USABLE + 1, g_norm2, d_slot))
        d_got = lax.all_to_all(d_slot, ALL, 0, 0, tiled=True)
        gains = lax.dynamic_slice_in_dim(jnp.sum(d_got[:, USABLE:], axis=0), me * shard, shard, axis=1).astype(BF16)
        n_slot = N_DEV * SLOTS
        key = jnp.where(slot_used, slot_row, rows_dev).reshape(-1)
        key_sorted, order = lax.sort((key, jnp.arange(n_slot, dtype=jnp.int32)), num_keys=1)
        edges = jnp.minimum(jnp.arange(pl.cdiv(rows_dev, ROW_BLOCK) + 1) * ROW_BLOCK, rows_dev)
        starts = jnp.sum((key[None, :] < edges[:, None]).astype(jnp.int32), axis=1)

        def rows_dense():
            d_all = [d_emb] + [lax.ppermute(d_emb, ALL, [(d, (d + k) % N_DEV) for d in range(N_DEV)]) for k in range(1, N_DEV)]
            d_all = jnp.concatenate(d_all, axis=0)
            origin = (me - jnp.arange(N_DEV)) % N_DEV
            seg = jnp.where(owner == me, rel, rows_dev)[origin].reshape(-1)
            return jax.ops.segment_sum(d_all.astype(F32), seg, num_segments=rows_dev).astype(BF16)

        d_rows = lax.cond(overflow, rows_dense, lambda: row_sums(starts, order, key_sorted, d_got.reshape(-1, dim), rows_dev))
        g_q = g_qkv[:, :q_w].reshape(w_query.shape)
        g_k = g_qkv[:, q_w : q_w + kv_w].reshape(w_key.shape)
        g_v = g_qkv[:, q_w + kv_w :].reshape(w_value.shape)
        return layer_out[None], d_rows, gains[0], gains[1], g_q, g_k, g_v, g_out, back[0], back[1], g_down


    return jax.shard_map(step, mesh=mesh, in_specs=in_specs, out_specs=out_specs, check_vma=False)
```

```python
import jax
import jax.numpy as jnp
from jax import lax
from jax.experimental import pallas as pl
from jax.experimental.pallas import tpu as pltpu
from jax.sharding import PartitionSpec as P


ALL = ("z", "y", "x", "c")
PLANE = ("z", "y")
N_DEV = 16
NORM_EPS = 1e-5
ROPE_THETA = 500000.0
SLOTS = 48
USABLE = SLOTS - 2
ROW_BLOCK = 128
CHUNKS = 2
F32 = jnp.float32
BF16 = jnp.bfloat16


def rms_norm(x_f32, gain_f32):
    inv_rms = lax.rsqrt(jnp.mean(x_f32 * x_f32, axis=-1, keepdims=True) + NORM_EPS)
    return (x_f32 * inv_rms * gain_f32).astype(BF16)


def rotary(x_f32):
    head_dim = x_f32.shape[-1]
    half_dim = head_dim // 2
    seq_len = x_f32.shape[-3]
    inv_freq = ROPE_THETA ** (-2.0 * jnp.arange(half_dim, dtype=F32) / head_dim)
    angles = jnp.arange(seq_len, dtype=F32)[:, None] * inv_freq[None, :]
    cos_tab = jnp.cos(angles)[:, None, :]
    sin_tab = jnp.sin(angles)[:, None, :]
    lo_half = x_f32[..., :half_dim]
    hi_half = x_f32[..., half_dim:]
    return jnp.concatenate([lo_half * cos_tab - hi_half * sin_tab, hi_half * cos_tab + lo_half * sin_tab], axis=-1)


def attend(q_f32, k_f32, v_bf16):
    batch_loc, seq_len, q_heads, head_dim = q_f32.shape
    kv_heads = k_f32.shape[2]
    q_rot = rotary(q_f32).astype(BF16).reshape(batch_loc, seq_len, kv_heads, q_heads // kv_heads, head_dim)
    k_rot = rotary(k_f32).astype(BF16)
    scores = jnp.einsum("bqkgd,bskd->bkgqs", q_rot, k_rot, preferred_element_type=F32) * head_dim ** -0.5
    positions = jnp.arange(seq_len)
    causal = positions[:, None] >= positions[None, :]
    scores = jnp.where(causal, scores, -1e30)
    prob_bf = jax.nn.softmax(scores, axis=-1).astype(BF16)
    attn_out = jnp.einsum("bkgqs,bskd->bqkgd", prob_bf, v_bf16, preferred_element_type=F32)
    return attn_out.astype(BF16).reshape(batch_loc, seq_len, q_heads * head_dim)


def gated(gate_f32, up_f32):
    return (jax.nn.silu(gate_f32) * up_f32).astype(BF16)


def dot(a, b, ca, cb):
    return lax.dot_general(a, b, (((ca,), (cb,)), ((), ())), preferred_element_type=F32)


def flip(a, axis):
    return lax.ppermute(a, axis, [(0, 1), (1, 0)])


def row_sum_kernel(start_ref, slot_ref, row_ref, recv_ref, out_ref, acc):
    blk = pl.program_id(0)
    acc[...] = jnp.zeros_like(acc)

    def add_row(i, carry):
        r = row_ref[i] - blk * ROW_BLOCK
        acc[pl.ds(r, 1), :] += recv_ref[pl.ds(slot_ref[i], 1), :]
        return carry

    lax.fori_loop(start_ref[blk], start_ref[blk + 1], add_row, 0)
    out_ref[...] = acc[...].astype(BF16)


def row_sums(starts, slots, rows, recv, rows_dev):
    width = recv.shape[1]
    n_blk = pl.cdiv(rows_dev, ROW_BLOCK)
    return pl.pallas_call(
        row_sum_kernel,
        out_shape=jax.ShapeDtypeStruct((rows_dev, width), BF16),
        grid_spec=pltpu.PrefetchScalarGridSpec(
            num_scalar_prefetch=3,
            grid=(n_blk,),
            in_specs=[pl.BlockSpec(recv.shape, lambda i, *_: (0, 0))],
            out_specs=pl.BlockSpec((ROW_BLOCK, width), lambda i, *_: (i, 0)),
            scratch_shapes=[pltpu.VMEM((ROW_BLOCK, width), F32)],
        ),
        compiler_params=pltpu.CompilerParams(dimension_semantics=("arbitrary",)),
        cost_estimate=pl.CostEstimate(flops=40_000_000_000, bytes_accessed=40_000_000, transcendentals=0),
    )(starts, slots, rows, recv)


def flipped(mask):
    here = [lax.axis_index(n) for n in ALL]
    return tuple(1 - v if (mask >> (3 - i)) & 1 else v for i, v in enumerate(here))


def share_kernel(in_ref, out_ref, send_sem, recv_sem):
    me = lax.axis_index(ALL)
    barrier = pltpu.get_barrier_semaphore()
    for m in range(1, N_DEV):
        pl.semaphore_signal(barrier, inc=1, device_id=flipped(m), device_id_type=pl.DeviceIdType.MESH)
    pl.semaphore_wait(barrier, N_DEV - 1)
    copies = []
    for m in range(1, N_DEV):
        copies.append(
            pltpu.make_async_remote_copy(
                src_ref=in_ref, dst_ref=out_ref.at[me], send_sem=send_sem.at[m], recv_sem=recv_sem.at[m], device_id=flipped(m), device_id_type=pl.DeviceIdType.MESH
            )
        )
        copies[-1].start()
    out_ref[me] = in_ref[...]
    for copy in copies:
        copy.wait()


def share(small):
    return pl.pallas_call(
        share_kernel,
        out_shape=jax.ShapeDtypeStruct((N_DEV,) + small.shape, small.dtype),
        in_specs=[pl.BlockSpec(memory_space=pltpu.VMEM)],
        out_specs=pl.BlockSpec(memory_space=pltpu.VMEM),
        scratch_shapes=[pltpu.SemaphoreType.DMA((N_DEV,)), pltpu.SemaphoreType.DMA((N_DEV,))],
        compiler_params=pltpu.CompilerParams(collective_id=0, has_side_effects=True),
        cost_estimate=pl.CostEstimate(flops=20_000_000, bytes_accessed=100_000, transcendentals=0),
    )(small)


def place_xc(pieces, x_i, c_i, shape, at):
    buf = jnp.zeros(shape, pieces[0].dtype)
    for k, piece in enumerate(pieces):
        px = x_i if k < 2 else 1 - x_i
        pc = c_i if k % 2 == 0 else 1 - c_i
        buf = lax.dynamic_update_slice(buf, piece, at(px, pc))
    return buf


def solution(mesh):
    mesh = jax.sharding.Mesh(mesh.devices.reshape(2, 2, 2, 2), ALL)
    spec_1d = P(ALL)
    spec_2d = P(ALL, None)
    spec_3d = P(ALL, None, None)
    in_specs = (spec_2d, spec_3d, spec_2d, spec_1d, spec_1d, spec_3d, spec_3d, spec_3d, spec_2d, spec_2d, spec_2d, spec_2d)
    out_specs = (spec_3d, spec_2d, spec_1d, spec_1d, spec_3d, spec_3d, spec_3d, spec_2d, spec_2d, spec_2d, spec_2d)

    def step(token_ids, grad_y, table, gain1, gain2, w_query, w_key, w_value, w_out, w_gate, w_up, w_down):
        seq = token_ids.shape[1]
        rows_dev, dim = table.shape
        shard = w_gate.shape[0]
        ffn = w_gate.shape[1]
        ffn_q = ffn // 4
        q_w = w_query.shape[1] * w_query.shape[2]
        kv_w = w_key.shape[1] * w_key.shape[2]
        qkv_w = q_w + 2 * kv_w
        me = lax.axis_index(ALL)
        x_i, c_i = lax.axis_index("x"), lax.axis_index("c")

        small = jnp.concatenate([token_ids[0].astype(F32), gain1.astype(F32), gain2.astype(F32), jnp.zeros((1024 - seq - 2 * shard,), F32)])
        small = share(small.reshape(8, 128))
        small = small.reshape(N_DEV, 1024)
        ids_all = small[:, :seq].astype(jnp.int32)
        g1_full = small[:, seq : seq + shard].reshape(-1)
        g2_full = small[:, seq + shard : seq + 2 * shard].reshape(-1)

        owner = ids_all // rows_dev
        pos = jnp.arange(seq)
        before = pos[None, :] < pos[:, None]
        same = ids_all[:, :, None] == ids_all[:, None, :]
        first = jnp.logical_not(jnp.any(same & before[None], axis=2))
        mine = first & (owner == me)
        owner_is = (owner[:, :, None] == jnp.arange(N_DEV)) & first[:, :, None]
        overflow = jnp.max(jnp.sum(owner_is.astype(jnp.int32), axis=1)) > USABLE
        rank = jnp.einsum("bt,st->bs", mine.astype(BF16), before.astype(BF16), preferred_element_type=F32).astype(jnp.int32)
        in_slot = mine[:, None, :] & (rank[:, None, :] == jnp.arange(SLOTS)[None, :, None])
        rel = ids_all - me * rows_dev
        slot_row = jnp.sum(jnp.where(in_slot, rel[:, None, :], 0), axis=2)
        slot_used = jnp.any(in_slot, axis=2)
        spread = (jnp.arange(N_DEV * SLOTS).reshape(N_DEV, SLOTS) * 12) % rows_dev
        fetch_row = jnp.where(slot_used, slot_row, spread)
        ids_me = token_ids[0]
        own_me = ids_me // rows_dev
        same_me = ids_me[:, None] == ids_me[None, :]
        first_me = jnp.logical_not(jnp.any(same_me & before, axis=1))
        rank_me = jnp.sum(((own_me[:, None] == own_me[None, :]) & before & first_me[None, :]).astype(jnp.int32), axis=1)
        slot_first = own_me * SLOTS + rank_me
        slot_tok = jnp.sum(jnp.where(same_me & first_me[None, :], slot_first[None, :], 0), axis=1)
        pick = (slot_tok[:, None] == jnp.arange(N_DEV * SLOTS)[None, :]).astype(BF16)

        sent = table.at[fetch_row.reshape(-1)].get(mode="promise_in_bounds").reshape(N_DEV, SLOTS, dim)
        got = lax.all_to_all(sent, ALL, 0, 0, tiled=True)
        emb_fast = dot(pick, got.reshape(-1, dim), 1, 0).astype(BF16)

        def emb_dense():
            owned = owner == me
            picked = jnp.take(table, jnp.where(owned, rel, 0), axis=0)
            part = jnp.where(owned[:, :, None], picked, jnp.zeros((), BF16))
            total = lax.dynamic_index_in_dim(part, me, 0, keepdims=False)
            for k in range(1, N_DEV):
                out = lax.dynamic_index_in_dim(part, (me + k) % N_DEV, 0, keepdims=False)
                total += lax.ppermute(out, ALL, [(d, (d + k) % N_DEV) for d in range(N_DEV)])
            return total

        emb = lax.cond(overflow, emb_dense, lambda: emb_fast)

        attn_w = jnp.concatenate([w_query.reshape(shard, -1), w_key.reshape(shard, -1), w_value.reshape(shard, -1), w_out], axis=1)
        attn_w = lax.all_gather(attn_w, ALL, axis=0, tiled=True)
        w_qkv, w_o = attn_w[:, :qkv_w], attn_w[:, qkv_w:]
        dy = grad_y[0]
        dy_all = lax.all_gather(dy, PLANE, axis=0, tiled=True)
        dy_all = dy_all.reshape(4, CHUNKS, -1, dim).transpose(1, 0, 2, 3).reshape(-1, dim)

        def gather_xc(w):
            wx = flip(w, "x")
            return [w, flip(w, "c"), wx, flip(wx, "c")]

        def wide(w):
            cols = jnp.stack([w[:, k * ffn_q : (k + 1) * ffn_q] for k in range(4)])
            cols = lax.all_to_all(cols, PLANE, 0, 0, tiled=True)
            pieces = [p[:, None, None] for p in gather_xc(cols)]
            return place_xc(pieces, x_i, c_i, (4, 2, 2, shard, ffn_q), lambda px, pc: (0, px, pc, 0, 0)).reshape(dim, ffn_q)

        w_d = place_xc([p[None, None] for p in gather_xc(w_down)], x_i, c_i, (2, 2) + w_down.shape, lambda px, pc: (px, pc, 0, 0)).reshape(ffn_q, dim)
        w_g = wide(w_gate)
        w_u = wide(w_up)

        x_f32 = emb.astype(F32)
        h_one, norm1_pull = jax.vjp(rms_norm, x_f32, g1_full)
        qkv = dot(h_one, w_qkv, 1, 0)
        q_f32 = qkv[:, :q_w].reshape(1, seq, -1, 128)
        k_f32 = qkv[:, q_w : q_w + kv_w].reshape(1, seq, -1, 128)
        v_bf16 = qkv[:, q_w + kv_w :].astype(BF16).reshape(1, seq, -1, 128)
        attn_out, attn_pull = jax.vjp(attend, q_f32, k_f32, v_bf16)
        o_bf = attn_out[0]
        resid_bf = (x_f32 + dot(o_bf, w_o, 1, 0)).astype(BF16)
        resid_two = resid_bf.astype(F32)
        h_two, norm2_pull = jax.vjp(rms_norm, resid_two, g2_full)

        step_t = seq // CHUNKS
        h_own = h_two.reshape(CHUNKS, step_t, dim)
        hs, acts, d_gates, d_ups, d_hs = [], [], [], [], []
        for k in range(CHUNKS):
            d_act = dot(lax.slice_in_dim(dy_all, k * 4 * step_t, (k + 1) * 4 * step_t), w_d, 1, 1).astype(BF16)
            h_k = lax.all_gather(h_own[k], PLANE, axis=0, tiled=True)
            gate_f32 = dot(h_k, w_g, 1, 0)
            up_f32 = dot(h_k, w_u, 1, 0)
            act_k, act_pull = jax.vjp(gated, gate_f32, up_f32)
            d_gate, d_up = act_pull(d_act)
            act_k, d_gate, d_up = lax.optimization_barrier((act_k, d_gate.astype(BF16), d_up.astype(BF16)))
            d_h_part = dot(d_gate, w_g, 1, 1) + dot(d_up, w_u, 1, 1)
            d_hs.append(lax.psum_scatter(d_h_part, PLANE, scatter_dimension=0, tiled=True).astype(BF16))
            hs.append(h_k)
            acts.append(act_k)
            d_gates.append(d_gate)
            d_ups.append(d_up)
        d_h_two = jnp.concatenate(d_hs)
        y_sums = []
        for k in range(CHUNKS):
            y_part = dot(acts[k], w_d, 1, 0)
            y_sums.append(lax.psum_scatter(y_part, PLANE, scatter_dimension=0, tiled=True))
        y_sum, resid_y = lax.optimization_barrier((jnp.concatenate(y_sums), resid_bf))
        layer_out = (resid_y.astype(F32) + y_sum).astype(BF16)
        h_all, d_gate, d_up = (jnp.concatenate(v) for v in (hs, d_gates, d_ups))
        act = jnp.concatenate(acts)

        def reduce_xc(part, c_dim, x_dim):
            keep = lax.dynamic_index_in_dim(part, c_i, c_dim, keepdims=False)
            give = lax.dynamic_index_in_dim(part, 1 - c_i, c_dim, keepdims=False)
            got_c = flip(give, "c")
            half = keep + got_c
            keep = lax.dynamic_index_in_dim(half, x_i, x_dim, keepdims=False)
            give = lax.dynamic_index_in_dim(half, 1 - x_i, x_dim, keepdims=False)
            got_x = flip(give, "x")
            return (keep + got_x).astype(BF16)

        g_gate = dot(h_all, d_gate, 0, 0)
        g_up = dot(h_all, d_up, 0, 0)
        g_down = dot(act, dy_all, 0, 0)
        g_gate = reduce_xc(g_gate.reshape(4, 2, 2, shard, ffn_q), 2, 1)
        g_up = reduce_xc(g_up.reshape(4, 2, 2, shard, ffn_q), 2, 1)
        g_down = reduce_xc(g_down.reshape(2, 2, ffn // N_DEV, dim), 1, 0)
        back = lax.all_to_all(jnp.stack([g_gate, g_up], axis=1), PLANE, 0, 0, tiled=True)
        back = back.transpose(1, 2, 0, 3).reshape(2, shard, ffn)

        d_resid_two, g_norm2 = norm2_pull(d_h_two)
        d_resid = (dy.astype(F32) + d_resid_two).astype(BF16)
        g_out = dot(o_bf, d_resid, 0, 0)
        g_out = lax.psum_scatter(g_out, ALL, scatter_dimension=0, tiled=True).astype(BF16)
        d_attn = dot(d_resid, w_o, 1, 1).astype(BF16)
        d_query, d_key, d_value = attn_pull(d_attn[None])
        d_qkv = jnp.concatenate([d_query.astype(BF16).reshape(seq, -1), d_key.astype(BF16).reshape(seq, -1), d_value.reshape(seq, -1)], axis=1)
        g_qkv = dot(h_one, d_qkv, 0, 0)
        g_qkv = lax.psum_scatter(g_qkv, ALL, scatter_dimension=0, tiled=True).astype(BF16)
        d_h_one = dot(d_qkv, w_qkv, 1, 1).astype(BF16)
        d_x, g_norm1 = norm1_pull(d_h_one)
        d_emb = (d_resid.astype(F32) + d_x).astype(BF16)

        d_slot = dot(pick, d_emb, 0, 0).reshape(N_DEV, SLOTS, dim)
        place = jnp.arange(SLOTS)[None, :, None]
        d_slot = jnp.where(place == USABLE, g_norm1, jnp.where(place == USABLE + 1, g_norm2, d_slot))
        d_got = lax.all_to_all(d_slot, ALL, 0, 0, tiled=True)
        gains = lax.dynamic_slice_in_dim(jnp.sum(d_got[:, USABLE:], axis=0), me * shard, shard, axis=1).astype(BF16)
        n_slot = N_DEV * SLOTS
        key = jnp.where(slot_used, slot_row, rows_dev).reshape(-1)
        key_sorted, order = lax.sort((key, jnp.arange(n_slot, dtype=jnp.int32)), num_keys=1)
        edges = jnp.minimum(jnp.arange(pl.cdiv(rows_dev, ROW_BLOCK) + 1) * ROW_BLOCK, rows_dev)
        starts = jnp.sum((key[None, :] < edges[:, None]).astype(jnp.int32), axis=1)

        def rows_dense():
            d_all = [d_emb] + [lax.ppermute(d_emb, ALL, [(d, (d + k) % N_DEV) for d in range(N_DEV)]) for k in range(1, N_DEV)]
            d_all = jnp.concatenate(d_all, axis=0)
            origin = (me - jnp.arange(N_DEV)) % N_DEV
            seg = jnp.where(owner == me, rel, rows_dev)[origin].reshape(-1)
            return jax.ops.segment_sum(d_all.astype(F32), seg, num_segments=rows_dev).astype(BF16)

        d_rows = lax.cond(overflow, rows_dense, lambda: row_sums(starts, order, key_sorted, d_got.reshape(-1, dim), rows_dev))
        g_q = g_qkv[:, :q_w].reshape(w_query.shape)
        g_k = g_qkv[:, q_w : q_w + kv_w].reshape(w_key.shape)
        g_v = g_qkv[:, q_w + kv_w :].reshape(w_value.shape)
        return layer_out[None], d_rows, gains[0], gains[1], g_q, g_k, g_v, g_out, back[0], back[1], g_down


    return jax.shard_map(step, mesh=mesh, in_specs=in_specs, out_specs=out_specs, check_vma=False)
```

```python
import jax
import jax.numpy as jnp
import numpy as np
from jax import lax
from jax.experimental import pallas as pl
from jax.experimental.pallas import tpu as pltpu
from jax.sharding import PartitionSpec as P


ALL = ("z", "y", "x", "c")
PLANE = ("z", "y")
N_DEV = 16
NORM_EPS = 1e-5
ROPE_THETA = 500000.0
SLOTS = 48
USABLE = SLOTS - 2
ROW_BLOCK = 512
CHUNKS = 2
F32 = jnp.float32
BF16 = jnp.bfloat16
MESH = pl.DeviceIdType.MESH


def rms_norm(x_f32, gain_f32):
    inv_rms = lax.rsqrt(jnp.mean(x_f32 * x_f32, axis=-1, keepdims=True) + NORM_EPS)
    return (x_f32 * inv_rms * gain_f32).astype(BF16)


def rotary(x_f32):
    head_dim = x_f32.shape[-1]
    half_dim = head_dim // 2
    seq_len = x_f32.shape[-3]
    inv_freq = np.float32(ROPE_THETA) ** (np.float32(-2.0) * np.arange(half_dim, dtype=np.float32) / np.float32(head_dim))
    angles = (np.arange(seq_len, dtype=np.float32)[:, None] * inv_freq[None, :]).astype(np.float32)
    cos_tab = jnp.asarray(np.cos(angles))[:, None, :]
    sin_tab = jnp.asarray(np.sin(angles))[:, None, :]
    lo_half = x_f32[..., :half_dim]
    hi_half = x_f32[..., half_dim:]
    return jnp.concatenate([lo_half * cos_tab - hi_half * sin_tab, hi_half * cos_tab + lo_half * sin_tab], axis=-1)


def attend(q_f32, k_f32, v_bf16):
    batch_loc, seq_len, q_heads, head_dim = q_f32.shape
    kv_heads = k_f32.shape[2]
    q_rot = rotary(q_f32).astype(BF16).reshape(batch_loc, seq_len, kv_heads, q_heads // kv_heads, head_dim)
    k_rot = rotary(k_f32).astype(BF16)
    scores = jnp.einsum("bqkgd,bskd->bkgqs", q_rot, k_rot, preferred_element_type=F32) * head_dim ** -0.5
    positions = jnp.arange(seq_len)
    causal = positions[:, None] >= positions[None, :]
    scores = jnp.where(causal, scores, -1e30)
    prob_bf = jax.nn.softmax(scores, axis=-1).astype(BF16)
    attn_out = jnp.einsum("bkgqs,bskd->bqkgd", prob_bf, v_bf16, preferred_element_type=F32)
    return attn_out.astype(BF16).reshape(batch_loc, seq_len, q_heads * head_dim)


def gated(gate_f32, up_f32):
    return (jax.nn.silu(gate_f32) * up_f32).astype(BF16)


def dot(a, b, ca, cb):
    return lax.dot_general(a, b, (((ca,), (cb,)), ((), ())), preferred_element_type=F32)


def flip(a, axis):
    return lax.ppermute(a, axis, [(0, 1), (1, 0)])


def pick_dim(a, index, dim):
    return lax.dynamic_index_in_dim(a, index, dim, keepdims=False)


def row_sum_kernel(start_ref, slot_ref, row_ref, recv_ref, out_ref, acc):
    blk = pl.program_id(0)
    acc[...] = jnp.zeros_like(acc)

    def add_row(i, carry):
        r = row_ref[i] - blk * ROW_BLOCK
        acc[pl.ds(r, 1), :] += recv_ref[pl.ds(slot_ref[i], 1), :]
        return carry

    lax.fori_loop(start_ref[blk], start_ref[blk + 1], add_row, 0)
    out_ref[...] = acc[...].astype(BF16)


def row_sums(starts, slots, rows, recv, rows_dev):
    width = recv.shape[1]
    n_blk = pl.cdiv(rows_dev, ROW_BLOCK)
    return pl.pallas_call(
        row_sum_kernel,
        out_shape=jax.ShapeDtypeStruct((rows_dev, width), BF16),
        grid_spec=pltpu.PrefetchScalarGridSpec(
            num_scalar_prefetch=3,
            grid=(n_blk,),
            in_specs=[pl.BlockSpec(recv.shape, lambda i, *_: (0, 0))],
            out_specs=pl.BlockSpec((ROW_BLOCK, width), lambda i, *_: (i, 0)),
            scratch_shapes=[pltpu.VMEM((ROW_BLOCK, width), F32)],
        ),
        cost_estimate=pl.CostEstimate(flops=40_000_000_000, bytes_accessed=40_000_000, transcendentals=0),
    )(starts, slots, rows, recv)


def flipped(mask):
    here = [lax.axis_index(n) for n in ALL]
    return tuple(1 - v if (mask >> (3 - i)) & 1 else v for i, v in enumerate(here))


def enter_all():
    barrier = pltpu.get_barrier_semaphore()
    for m in range(1, N_DEV):
        pl.semaphore_signal(barrier, inc=1, device_id=flipped(m), device_id_type=MESH)
    pl.semaphore_wait(barrier, N_DEV - 1)


def share_kernel(in_ref, out_ref, send_sem, recv_sem):
    me = lax.axis_index(ALL)
    enter_all()
    copies = []
    for m in range(1, N_DEV):
        copies.append(
            pltpu.make_async_remote_copy(
                src_ref=in_ref, dst_ref=out_ref.at[me], send_sem=send_sem.at[m], recv_sem=recv_sem.at[m], device_id=flipped(m), device_id_type=MESH
            )
        )
        copies[-1].start()
    out_ref[me] = in_ref[...]
    for copy in copies:
        copy.wait()


def exchange(kernel, array, out_shape, collective_id, flops):
    return pl.pallas_call(
        kernel,
        out_shape=jax.ShapeDtypeStruct(out_shape, array.dtype),
        in_specs=[pl.BlockSpec(memory_space=pltpu.VMEM)],
        out_specs=pl.BlockSpec(memory_space=pltpu.VMEM),
        scratch_shapes=[pltpu.SemaphoreType.DMA((N_DEV,)), pltpu.SemaphoreType.DMA((N_DEV,))],
        compiler_params=pltpu.CompilerParams(collective_id=collective_id, has_side_effects=True),
        cost_estimate=pl.CostEstimate(flops=flops, bytes_accessed=2 * array.size, transcendentals=0),
    )(array)


def pair_kernel(own_ref, far_ref, out_ref, local_sem, send_sem, recv_sem):
    x_i, c_i = lax.axis_index("x"), lax.axis_index("c")
    other = flipped(1)
    barrier = pltpu.get_barrier_semaphore()
    pl.semaphore_signal(barrier, inc=1, device_id=other, device_id_type=MESH)
    pl.semaphore_wait(barrier, 1)
    copies = []
    for k, (ref, px) in enumerate(((own_ref, x_i), (far_ref, 1 - x_i))):
        to = out_ref.at[:, px, c_i]
        copies.append(
            pltpu.make_async_remote_copy(src_ref=ref, dst_ref=to, send_sem=send_sem.at[k], recv_sem=recv_sem.at[k], device_id=other, device_id_type=MESH)
        )
        copies.append(pltpu.make_async_copy(ref, to, local_sem.at[k]))
    for copy in copies:
        copy.start()
    for copy in copies:
        copy.wait()


def gather_xc(w, collective_id):
    far = flip(w, "x")
    a, r, n = w.shape
    return pl.pallas_call(
        pair_kernel,
        out_shape=jax.ShapeDtypeStruct((a, 2, 2, r, n), w.dtype),
        in_specs=[pl.BlockSpec(memory_space=pltpu.VMEM)] * 2,
        out_specs=pl.BlockSpec(memory_space=pl.ANY),
        scratch_shapes=[pltpu.SemaphoreType.DMA((2,))] * 3,
        compiler_params=pltpu.CompilerParams(collective_id=collective_id, has_side_effects=True),
        cost_estimate=pl.CostEstimate(flops=60_000_000, bytes_accessed=8 * w.size, transcendentals=0),
    )(w, far)


def solution(mesh):
    mesh = jax.sharding.Mesh(mesh.devices.reshape(2, 2, 2, 2), ALL)
    spec_1d = P(ALL)
    spec_2d = P(ALL, None)
    spec_3d = P(ALL, None, None)
    in_specs = (spec_2d, spec_3d, spec_2d, spec_1d, spec_1d, spec_3d, spec_3d, spec_3d, spec_2d, spec_2d, spec_2d, spec_2d)
    out_specs = (spec_3d, spec_2d, spec_1d, spec_1d, spec_3d, spec_3d, spec_3d, spec_2d, spec_2d, spec_2d, spec_2d)

    def step(token_ids, grad_y, table, gain1, gain2, w_query, w_key, w_value, w_out, w_gate, w_up, w_down):
        seq = token_ids.shape[1]
        rows_dev, dim = table.shape
        shard = w_gate.shape[0]
        ffn = w_gate.shape[1]
        ffn_q = ffn // 4
        q_w = w_query.shape[1] * w_query.shape[2]
        kv_w = w_key.shape[1] * w_key.shape[2]
        step_t = seq // CHUNKS
        me = lax.axis_index(ALL)
        z_i, y_i, x_i, c_i = (lax.axis_index(n) for n in ALL)

        small = jnp.concatenate([token_ids[0].astype(F32), gain1.astype(F32), gain2.astype(F32), jnp.zeros((1024 - seq - 2 * shard,), F32)])
        small = exchange(share_kernel, small.reshape(8, 128), (N_DEV, 8, 128), 0, 20_000_000)
        small = small.reshape(N_DEV, 1024)
        ids_all = small[:, :seq].astype(jnp.int32)
        g1_full = small[:, seq : seq + shard].reshape(-1)
        g2_full = small[:, seq + shard : seq + 2 * shard].reshape(-1)

        owner = ids_all // rows_dev
        pos = jnp.arange(seq)
        before = pos[None, :] < pos[:, None]
        same = ids_all[:, :, None] == ids_all[:, None, :]
        first = jnp.logical_not(jnp.any(same & before[None], axis=2))
        mine = first & (owner == me)
        owner_is = (owner[:, :, None] == jnp.arange(N_DEV)) & first[:, :, None]
        overflow = jnp.max(jnp.sum(owner_is.astype(jnp.int32), axis=1)) > USABLE
        rank = dot(mine.astype(BF16), before.astype(BF16), 1, 1).astype(jnp.int32)
        in_slot = mine[:, None, :] & (rank[:, None, :] == jnp.arange(SLOTS)[None, :, None])
        rel = ids_all - me * rows_dev
        slot_row = jnp.sum(jnp.where(in_slot, rel[:, None, :], 0), axis=2)
        slot_used = jnp.any(in_slot, axis=2)
        spread = (jnp.arange(N_DEV * SLOTS).reshape(N_DEV, SLOTS) * 12) % rows_dev
        fetch_row = jnp.where(slot_used, slot_row, spread)
        ids_me = token_ids[0]
        own_me = ids_me // rows_dev
        same_me = ids_me[:, None] == ids_me[None, :]
        first_me = jnp.logical_not(jnp.any(same_me & before, axis=1))
        rank_me = jnp.sum(((own_me[:, None] == own_me[None, :]) & before & first_me[None, :]).astype(jnp.int32), axis=1)
        slot_first = own_me * SLOTS + rank_me
        slot_tok = jnp.sum(jnp.where(same_me & first_me[None, :], slot_first[None, :], 0), axis=1)
        pick = (slot_tok[:, None] == jnp.arange(N_DEV * SLOTS)[None, :]).astype(BF16)

        sent = table.at[fetch_row.reshape(-1)].get(mode="promise_in_bounds").reshape(N_DEV, SLOTS, dim)
        got = lax.all_to_all(sent, ALL, 0, 0, tiled=True)
        emb_fast = dot(pick, got.reshape(-1, dim), 1, 0).astype(BF16)

        def ring(k):
            return [(d, (d + k) % N_DEV) for d in range(N_DEV)]

        def emb_dense():
            owned = owner == me
            picked = jnp.take(table, jnp.where(owned, rel, 0), axis=0)
            part = jnp.where(owned[:, :, None], picked, jnp.zeros((), BF16))
            total = pick_dim(part, me, 0)
            for k in range(1, N_DEV):
                total += lax.ppermute(pick_dim(part, (me + k) % N_DEV, 0), ALL, ring(k))
            return total

        emb = lax.cond(overflow, emb_dense, lambda: emb_fast)

        w_qkv = jnp.concatenate([w_query.reshape(shard, -1), w_key.reshape(shard, -1), w_value.reshape(shard, -1)], axis=1)
        w_qkv = lax.all_gather(w_qkv, ALL, axis=0, tiled=True)
        w_o = lax.all_gather(w_out, ALL, axis=0, tiled=True)
        dy = grad_y[0]
        dy_z, dy_y = flip(dy, "z"), flip(dy, "y")
        dy_far = jnp.concatenate([flip(dy_z[:, : dim // 2], "y"), flip(dy_y[:, dim // 2 :], "z")], axis=1)
        dys = lax.dynamic_update_slice(jnp.zeros((CHUNKS, 2, 2, step_t, dim), BF16), dy.reshape(CHUNKS, 1, 1, step_t, dim), (0, z_i, y_i, 0, 0))
        for block, at_z, at_y in ((dy_z, 1 - z_i, y_i), (dy_y, z_i, 1 - y_i), (dy_far, 1 - z_i, 1 - y_i)):
            dys = lax.dynamic_update_slice(dys, block.reshape(CHUNKS, 1, 1, step_t, dim), (0, at_z, at_y, 0, 0))
        dys = dys.reshape(CHUNKS, 4 * step_t, dim)

        def wide(w, collective_id):
            cols = jnp.stack([w[:, k * ffn_q : (k + 1) * ffn_q] for k in range(4)])
            cols = lax.all_to_all(cols, PLANE, 0, 0, tiled=True)
            return gather_xc(cols, collective_id).reshape(dim, ffn_q)

        w_d = gather_xc(w_down[None], 2).reshape(ffn_q, dim)
        w_g = wide(w_gate, 3)
        w_u = wide(w_up, 4)

        x_f32 = emb.astype(F32)
        h_one, norm1_pull = jax.vjp(rms_norm, x_f32, g1_full)
        qkv = dot(h_one, w_qkv, 1, 0)
        q_f32 = qkv[:, :q_w].reshape(1, seq, -1, 128)
        k_f32 = qkv[:, q_w : q_w + kv_w].reshape(1, seq, -1, 128)
        v_bf16 = qkv[:, q_w + kv_w :].astype(BF16).reshape(1, seq, -1, 128)
        attn_out, attn_pull = jax.vjp(attend, q_f32, k_f32, v_bf16)
        o_bf = attn_out[0]
        resid_bf = (x_f32 + dot(o_bf, w_o, 1, 0)).astype(BF16)
        resid_two = resid_bf.astype(F32)
        h_two, norm2_pull = jax.vjp(rms_norm, resid_two, g2_full)

        def add_flip(part, index, dim_at, axis, cols=slice(None)):
            keep, give = pick_dim(part, index, dim_at)[..., cols], pick_dim(part, 1 - index, dim_at)[..., cols]
            got_half = flip(give, axis)
            return keep + got_half

        def plane_sum(part):
            part = lax.optimization_barrier(part).reshape(2, 2, -1, dim)
            a = add_flip(part, z_i, 0, "z", slice(dim // 2))
            b = add_flip(part, y_i, 1, "y", slice(dim // 2, dim))
            return jnp.concatenate([add_flip(a, y_i, 0, "y"), add_flip(b, z_i, 0, "z")], axis=1)

        hs, acts, d_gates, d_ups, d_hs, y_sums = [], [], [], [], [], []
        for k in range(CHUNKS):
            h_k = lax.all_gather(h_two[k * step_t : (k + 1) * step_t], PLANE, axis=0, tiled=True)
            d_act = dot(dys[k], w_d, 1, 1).astype(BF16)
            up_f32 = dot(h_k, w_u, 1, 0)
            gate_f32 = dot(h_k, w_g, 1, 0)
            act_k, act_pull = jax.vjp(gated, gate_f32, up_f32)
            d_gate, d_up = act_pull(d_act)
            act_k, d_gate, d_up = lax.optimization_barrier((act_k, d_gate.astype(BF16), d_up.astype(BF16)))
            d_h_part = dot(d_gate, w_g, 1, 1) + dot(d_up, w_u, 1, 1)
            d_hs.append(lax.psum_scatter(d_h_part, PLANE, scatter_dimension=0, tiled=True).astype(BF16))
            y_part = dot(act_k, w_d, 1, 0)
            y_sums.append(plane_sum(y_part))
            hs.append(h_k)
            acts.append(act_k)
            d_gates.append(d_gate)
            d_ups.append(d_up)
        d_h_two = jnp.concatenate(d_hs)
        y_sum, resid_y = lax.optimization_barrier((jnp.concatenate(y_sums), resid_bf))
        layer_out = (resid_y.astype(F32) + y_sum).astype(BF16)
        h_all, d_gate, d_up = (jnp.concatenate(v) for v in (hs, d_gates, d_ups))
        act, dy_all = jnp.concatenate(acts), dys.reshape(-1, dim)

        def grad_xc(a, b, shape, c_dim):
            part = dot(a, b, 0, 0).reshape(shape)
            half = add_flip(part, c_i, c_dim, "c")
            return add_flip(half, x_i, c_dim - 1, "x").astype(BF16)

        def grad_all(a, b):
            part = dot(a, b, 0, 0).reshape(4, 2, 2, shard, -1)
            half = add_flip(part, c_i, 2, "c")
            half = lax.psum_scatter(half.reshape(8 * shard, -1), PLANE, scatter_dimension=0, tiled=True)
            return add_flip(half.reshape(2, shard, -1), x_i, 0, "x").astype(BF16)

        cols = (4, 2, 2, shard, ffn_q)
        g_gate = grad_xc(h_all, d_gate, cols, 2)
        g_up = grad_xc(h_all, d_up, cols, 2)
        g_down = grad_xc(act, dy_all, (2, 2, ffn // N_DEV, dim), 1)
        back = lax.all_to_all(jnp.stack([g_gate, g_up], axis=1), PLANE, 0, 0, tiled=True)
        back = back.transpose(1, 2, 0, 3).reshape(2, shard, ffn)

        d_resid_two, g_norm2 = norm2_pull(d_h_two)
        d_resid = (dy.astype(F32) + d_resid_two).astype(BF16)
        g_out = grad_all(o_bf, d_resid)
        d_attn = dot(d_resid, w_o, 1, 1).astype(BF16)
        d_query, d_key, d_value = attn_pull(d_attn[None])
        d_qkv = jnp.concatenate([d_query.astype(BF16).reshape(seq, -1), d_key.astype(BF16).reshape(seq, -1), d_value.reshape(seq, -1)], axis=1)
        g_qkv = grad_all(h_one, d_qkv)
        d_h_one = dot(d_qkv, w_qkv, 1, 1).astype(BF16)
        d_x, g_norm1 = norm1_pull(d_h_one)
        d_emb = (d_resid.astype(F32) + d_x).astype(BF16)

        d_slot = dot(pick, d_emb, 0, 0).reshape(N_DEV, SLOTS, dim)
        place = jnp.arange(SLOTS)[None, :, None]
        d_slot = jnp.where(place == USABLE, g_norm1, jnp.where(place == USABLE + 1, g_norm2, d_slot))
        d_got = lax.all_to_all(d_slot, ALL, 0, 0, tiled=True)
        gains = lax.dynamic_slice_in_dim(jnp.sum(d_got[:, USABLE:], axis=0), me * shard, shard, axis=1).astype(BF16)
        n_slot = N_DEV * SLOTS
        key = jnp.where(slot_used, slot_row, rows_dev).reshape(-1)
        key_sorted, order = lax.sort((key, jnp.arange(n_slot, dtype=jnp.int32)), num_keys=1)
        edges = jnp.minimum(jnp.arange(pl.cdiv(rows_dev, ROW_BLOCK) + 1) * ROW_BLOCK, rows_dev)
        starts = jnp.sum((key[None, :] < edges[:, None]).astype(jnp.int32), axis=1)

        def rows_dense():
            d_all = jnp.concatenate([d_emb] + [lax.ppermute(d_emb, ALL, ring(k)) for k in range(1, N_DEV)])
            origin = (me - jnp.arange(N_DEV)) % N_DEV
            seg = jnp.where(owner == me, rel, rows_dev)[origin].reshape(-1)
            return jax.ops.segment_sum(d_all.astype(F32), seg, num_segments=rows_dev).astype(BF16)

        d_rows = lax.cond(overflow, rows_dense, lambda: row_sums(starts, order, key_sorted, d_got.reshape(-1, dim), rows_dev))
        g_q = g_qkv[:, :q_w].reshape(w_query.shape)
        g_k = g_qkv[:, q_w : q_w + kv_w].reshape(w_key.shape)
        g_v = g_qkv[:, q_w + kv_w :].reshape(w_value.shape)
        return layer_out[None], d_rows, gains[0], gains[1], g_q, g_k, g_v, g_out, back[0], back[1], g_down

    return jax.shard_map(step, mesh=mesh, in_specs=in_specs, out_specs=out_specs, check_vma=False)
```

```python
import jax
import jax.numpy as jnp
import numpy as np
from jax import lax
from jax.experimental import pallas as pl
from jax.experimental.pallas import tpu as pltpu
from jax.sharding import PartitionSpec as P


ALL = ("z", "y", "x", "c")
PLANE = ("z", "y")
N_DEV = 16
NORM_EPS = 1e-5
ROPE_THETA = 500000.0
SLOTS = 48
USABLE = SLOTS - 2
ROW_BLOCK = 512
CHUNKS = 2
F32 = jnp.float32
BF16 = jnp.bfloat16
MESH = pl.DeviceIdType.MESH


def rms_norm(x_f32, gain_f32):
    inv_rms = lax.rsqrt(jnp.mean(x_f32 * x_f32, axis=-1, keepdims=True) + NORM_EPS)
    return (x_f32 * inv_rms * gain_f32).astype(BF16)


def rotary(x_f32):
    head_dim = x_f32.shape[-1]
    half_dim = head_dim // 2
    seq_len = x_f32.shape[-3]
    inv_freq = np.float32(ROPE_THETA) ** (np.float32(-2.0) * np.arange(half_dim, dtype=np.float32) / np.float32(head_dim))
    angles = (np.arange(seq_len, dtype=np.float32)[:, None] * inv_freq[None, :]).astype(np.float32)
    cos_tab = jnp.asarray(np.cos(angles))[:, None, :]
    sin_tab = jnp.asarray(np.sin(angles))[:, None, :]
    lo_half = x_f32[..., :half_dim]
    hi_half = x_f32[..., half_dim:]
    return jnp.concatenate([lo_half * cos_tab - hi_half * sin_tab, hi_half * cos_tab + lo_half * sin_tab], axis=-1)


def attend(q_f32, k_f32, v_bf16):
    batch_loc, seq_len, q_heads, head_dim = q_f32.shape
    kv_heads = k_f32.shape[2]
    q_rot = rotary(q_f32).astype(BF16).reshape(batch_loc, seq_len, kv_heads, q_heads // kv_heads, head_dim)
    k_rot = rotary(k_f32).astype(BF16)
    scores = jnp.einsum("bqkgd,bskd->bkgqs", q_rot, k_rot, preferred_element_type=F32) * head_dim ** -0.5
    positions = jnp.arange(seq_len)
    causal = positions[:, None] >= positions[None, :]
    scores = jnp.where(causal, scores, -1e30)
    prob_bf = jax.nn.softmax(scores, axis=-1).astype(BF16)
    attn_out = jnp.einsum("bkgqs,bskd->bqkgd", prob_bf, v_bf16, preferred_element_type=F32)
    return attn_out.astype(BF16).reshape(batch_loc, seq_len, q_heads * head_dim)


def gated(gate_f32, up_f32):
    return (jax.nn.silu(gate_f32) * up_f32).astype(BF16)


def dot(a, b, ca, cb):
    return lax.dot_general(a, b, (((ca,), (cb,)), ((), ())), preferred_element_type=F32)


def flip(a, axis):
    return lax.ppermute(a, axis, [(0, 1), (1, 0)])


def pick_dim(a, index, dim):
    return lax.dynamic_index_in_dim(a, index, dim, keepdims=False)


def row_sum_kernel(start_ref, slot_ref, row_ref, recv_ref, out_ref, acc):
    blk = pl.program_id(0)
    acc[...] = jnp.zeros_like(acc)

    def add_row(i, carry):
        r = row_ref[i] - blk * ROW_BLOCK
        acc[pl.ds(r, 1), :] += recv_ref[pl.ds(slot_ref[i], 1), :]
        return carry

    lax.fori_loop(start_ref[blk], start_ref[blk + 1], add_row, 0)
    out_ref[...] = acc[...].astype(BF16)


def row_sums(starts, slots, rows, recv, rows_dev):
    width = recv.shape[1]
    n_blk = pl.cdiv(rows_dev, ROW_BLOCK)
    return pl.pallas_call(
        row_sum_kernel,
        out_shape=jax.ShapeDtypeStruct((rows_dev, width), BF16),
        grid_spec=pltpu.PrefetchScalarGridSpec(
            num_scalar_prefetch=3,
            grid=(n_blk,),
            in_specs=[pl.BlockSpec(recv.shape, lambda i, *_: (0, 0))],
            out_specs=pl.BlockSpec((ROW_BLOCK, width), lambda i, *_: (i, 0)),
            scratch_shapes=[pltpu.VMEM((ROW_BLOCK, width), F32)],
        ),
        cost_estimate=pl.CostEstimate(flops=40_000_000_000, bytes_accessed=40_000_000, transcendentals=0),
    )(starts, slots, rows, recv)


def flipped(mask):
    here = [lax.axis_index(n) for n in ALL]
    return tuple(1 - v if (mask >> (3 - i)) & 1 else v for i, v in enumerate(here))


def enter_all():
    barrier = pltpu.get_barrier_semaphore()
    for m in range(1, N_DEV):
        pl.semaphore_signal(barrier, inc=1, device_id=flipped(m), device_id_type=MESH)
    pl.semaphore_wait(barrier, N_DEV - 1)


def share_kernel(in_ref, out_ref, send_sem, recv_sem):
    me = lax.axis_index(ALL)
    enter_all()
    copies = []
    for m in range(1, N_DEV):
        copies.append(
            pltpu.make_async_remote_copy(
                src_ref=in_ref, dst_ref=out_ref.at[me], send_sem=send_sem.at[m], recv_sem=recv_sem.at[m], device_id=flipped(m), device_id_type=MESH
            )
        )
        copies[-1].start()
    out_ref[me] = in_ref[...]
    for copy in copies:
        copy.wait()


def swap_kernel(in_ref, out_ref, send_sem, recv_sem):
    me = lax.axis_index(ALL)
    enter_all()
    copies = []
    for m in range(N_DEV - 1, 0, -1):
        z, y, x, c = flipped(m)
        to = ((z * 2 + y) * 2 + x) * 2 + c
        copies.append(
            pltpu.make_async_remote_copy(
                src_ref=in_ref.at[to], dst_ref=out_ref.at[me], send_sem=send_sem.at[m], recv_sem=recv_sem.at[m], device_id=(z, y, x, c), device_id_type=MESH
            )
        )
        copies[-1].start()
    out_ref[me] = in_ref[me]
    for copy in copies:
        copy.wait()


def exchange(kernel, array, out_shape, collective_id, flops):
    return pl.pallas_call(
        kernel,
        out_shape=jax.ShapeDtypeStruct(out_shape, array.dtype),
        in_specs=[pl.BlockSpec(memory_space=pltpu.VMEM)],
        out_specs=pl.BlockSpec(memory_space=pltpu.VMEM),
        scratch_shapes=[pltpu.SemaphoreType.DMA((N_DEV,)), pltpu.SemaphoreType.DMA((N_DEV,))],
        compiler_params=pltpu.CompilerParams(collective_id=collective_id, has_side_effects=True),
        cost_estimate=pl.CostEstimate(flops=flops, bytes_accessed=2 * array.size, transcendentals=0),
    )(array)


def pair_kernel(own_ref, far_ref, out_ref, local_sem, send_sem, recv_sem):
    x_i, c_i = lax.axis_index("x"), lax.axis_index("c")
    other = flipped(1)
    barrier = pltpu.get_barrier_semaphore()
    pl.semaphore_signal(barrier, inc=1, device_id=other, device_id_type=MESH)
    pl.semaphore_wait(barrier, 1)
    copies = []
    for k, (ref, px) in enumerate(((own_ref, x_i), (far_ref, 1 - x_i))):
        to = out_ref.at[:, px, c_i]
        copies.append(
            pltpu.make_async_remote_copy(src_ref=ref, dst_ref=to, send_sem=send_sem.at[k], recv_sem=recv_sem.at[k], device_id=other, device_id_type=MESH)
        )
        copies.append(pltpu.make_async_copy(ref, to, local_sem.at[k]))
    for copy in copies:
        copy.start()
    for copy in copies:
        copy.wait()


def gather_xc(w, collective_id):
    far = flip(w, "x")
    a, r, n = w.shape
    return pl.pallas_call(
        pair_kernel,
        out_shape=jax.ShapeDtypeStruct((a, 2, 2, r, n), w.dtype),
        in_specs=[pl.BlockSpec(memory_space=pltpu.VMEM)] * 2,
        out_specs=pl.BlockSpec(memory_space=pl.ANY),
        scratch_shapes=[pltpu.SemaphoreType.DMA((2,))] * 3,
        compiler_params=pltpu.CompilerParams(collective_id=collective_id, has_side_effects=True),
        cost_estimate=pl.CostEstimate(flops=60_000_000, bytes_accessed=8 * w.size, transcendentals=0),
    )(w, far)


def solution(mesh):
    mesh = jax.sharding.Mesh(mesh.devices.reshape(2, 2, 2, 2), ALL)
    spec_1d = P(ALL)
    spec_2d = P(ALL, None)
    spec_3d = P(ALL, None, None)
    in_specs = (spec_2d, spec_3d, spec_2d, spec_1d, spec_1d, spec_3d, spec_3d, spec_3d, spec_2d, spec_2d, spec_2d, spec_2d)
    out_specs = (spec_3d, spec_2d, spec_1d, spec_1d, spec_3d, spec_3d, spec_3d, spec_2d, spec_2d, spec_2d, spec_2d)

    def step(token_ids, grad_y, table, gain1, gain2, w_query, w_key, w_value, w_out, w_gate, w_up, w_down):
        seq = token_ids.shape[1]
        rows_dev, dim = table.shape
        shard = w_gate.shape[0]
        ffn = w_gate.shape[1]
        ffn_q = ffn // 4
        q_w = w_query.shape[1] * w_query.shape[2]
        kv_w = w_key.shape[1] * w_key.shape[2]
        step_t = seq // CHUNKS
        me = lax.axis_index(ALL)
        z_i, y_i, x_i, c_i = (lax.axis_index(n) for n in ALL)

        small = jnp.concatenate([token_ids[0].astype(F32), gain1.astype(F32), gain2.astype(F32), jnp.zeros((1024 - seq - 2 * shard,), F32)])
        small = exchange(share_kernel, small.reshape(8, 128), (N_DEV, 8, 128), 0, 20_000_000)
        small = small.reshape(N_DEV, 1024)
        ids_all = small[:, :seq].astype(jnp.int32)
        g1_full = small[:, seq : seq + shard].reshape(-1)
        g2_full = small[:, seq + shard : seq + 2 * shard].reshape(-1)

        owner = ids_all // rows_dev
        pos = jnp.arange(seq)
        before = pos[None, :] < pos[:, None]
        same = ids_all[:, :, None] == ids_all[:, None, :]
        first = jnp.logical_not(jnp.any(same & before[None], axis=2))
        mine = first & (owner == me)
        owner_is = (owner[:, :, None] == jnp.arange(N_DEV)) & first[:, :, None]
        overflow = jnp.max(jnp.sum(owner_is.astype(jnp.int32), axis=1)) > USABLE
        rank = dot(mine.astype(BF16), before.astype(BF16), 1, 1).astype(jnp.int32)
        in_slot = mine[:, None, :] & (rank[:, None, :] == jnp.arange(SLOTS)[None, :, None])
        rel = ids_all - me * rows_dev
        slot_row = jnp.sum(jnp.where(in_slot, rel[:, None, :], 0), axis=2)
        slot_used = jnp.any(in_slot, axis=2)
        spread = (jnp.arange(N_DEV * SLOTS).reshape(N_DEV, SLOTS) * 12) % rows_dev
        fetch_row = jnp.where(slot_used, slot_row, spread)
        ids_me = token_ids[0]
        own_me = ids_me // rows_dev
        same_me = ids_me[:, None] == ids_me[None, :]
        first_me = jnp.logical_not(jnp.any(same_me & before, axis=1))
        rank_me = jnp.sum(((own_me[:, None] == own_me[None, :]) & before & first_me[None, :]).astype(jnp.int32), axis=1)
        slot_first = own_me * SLOTS + rank_me
        slot_tok = jnp.sum(jnp.where(same_me & first_me[None, :], slot_first[None, :], 0), axis=1)
        pick = (slot_tok[:, None] == jnp.arange(N_DEV * SLOTS)[None, :]).astype(BF16)

        sent = table.at[fetch_row.reshape(-1)].get(mode="promise_in_bounds").reshape(N_DEV, SLOTS, dim)
        got = exchange(swap_kernel, sent, sent.shape, 1, 100_000_000)
        emb_fast = dot(pick, got.reshape(-1, dim), 1, 0).astype(BF16)

        def ring(k):
            return [(d, (d + k) % N_DEV) for d in range(N_DEV)]

        def emb_dense():
            owned = owner == me
            picked = jnp.take(table, jnp.where(owned, rel, 0), axis=0)
            part = jnp.where(owned[:, :, None], picked, jnp.zeros((), BF16))
            total = pick_dim(part, me, 0)
            for k in range(1, N_DEV):
                total += lax.ppermute(pick_dim(part, (me + k) % N_DEV, 0), ALL, ring(k))
            return total

        emb = lax.cond(overflow, emb_dense, lambda: emb_fast)

        w_qkv = jnp.concatenate([w_query.reshape(shard, -1), w_key.reshape(shard, -1), w_value.reshape(shard, -1)], axis=1)
        w_qkv = lax.all_gather(w_qkv, ALL, axis=0, tiled=True)
        w_o = lax.all_gather(w_out, ALL, axis=0, tiled=True)
        dy = grad_y[0]
        dy_z, dy_y = flip(dy, "z"), flip(dy, "y")
        dy_far = jnp.concatenate([flip(dy_z[:, : dim // 2], "y"), flip(dy_y[:, dim // 2 :], "z")], axis=1)
        dys = lax.dynamic_update_slice(jnp.zeros((CHUNKS, 2, 2, step_t, dim), BF16), dy.reshape(CHUNKS, 1, 1, step_t, dim), (0, z_i, y_i, 0, 0))
        for block, at_z, at_y in ((dy_z, 1 - z_i, y_i), (dy_y, z_i, 1 - y_i), (dy_far, 1 - z_i, 1 - y_i)):
            dys = lax.dynamic_update_slice(dys, block.reshape(CHUNKS, 1, 1, step_t, dim), (0, at_z, at_y, 0, 0))
        dys = dys.reshape(CHUNKS, 4 * step_t, dim)

        def wide(w, collective_id):
            cols = jnp.stack([w[:, k * ffn_q : (k + 1) * ffn_q] for k in range(4)])
            cols = lax.all_to_all(cols, PLANE, 0, 0, tiled=True)
            return gather_xc(cols, collective_id).reshape(dim, ffn_q)

        w_d = gather_xc(w_down[None], 2).reshape(ffn_q, dim)
        w_g = wide(w_gate, 3)
        w_u = wide(w_up, 4)

        x_f32 = emb.astype(F32)
        h_one, norm1_pull = jax.vjp(rms_norm, x_f32, g1_full)
        qkv = dot(h_one, w_qkv, 1, 0)
        q_f32 = qkv[:, :q_w].reshape(1, seq, -1, 128)
        k_f32 = qkv[:, q_w : q_w + kv_w].reshape(1, seq, -1, 128)
        v_bf16 = qkv[:, q_w + kv_w :].astype(BF16).reshape(1, seq, -1, 128)
        attn_out, attn_pull = jax.vjp(attend, q_f32, k_f32, v_bf16)
        o_bf = attn_out[0]
        resid_bf = (x_f32 + dot(o_bf, w_o, 1, 0)).astype(BF16)
        resid_two = resid_bf.astype(F32)
        h_two, norm2_pull = jax.vjp(rms_norm, resid_two, g2_full)

        def add_flip(part, index, dim_at, axis, cols=slice(None)):
            keep, give = pick_dim(part, index, dim_at)[..., cols], pick_dim(part, 1 - index, dim_at)[..., cols]
            got_half = flip(give, axis)
            return keep + got_half

        def plane_sum(part):
            part = lax.optimization_barrier(part).reshape(2, 2, -1, dim)
            a = add_flip(part, z_i, 0, "z", slice(dim // 2))
            b = add_flip(part, y_i, 1, "y", slice(dim // 2, dim))
            return jnp.concatenate([add_flip(a, y_i, 0, "y"), add_flip(b, z_i, 0, "z")], axis=1)

        hs, acts, d_gates, d_ups, d_hs, y_sums = [], [], [], [], [], []
        for k in range(CHUNKS):
            h_k = lax.all_gather(h_two[k * step_t : (k + 1) * step_t], PLANE, axis=0, tiled=True)
            d_act = dot(dys[k], w_d, 1, 1).astype(BF16)
            up_f32 = dot(h_k, w_u, 1, 0)
            gate_f32 = dot(h_k, w_g, 1, 0)
            act_k, act_pull = jax.vjp(gated, gate_f32, up_f32)
            d_gate, d_up = act_pull(d_act)
            act_k, d_gate, d_up = lax.optimization_barrier((act_k, d_gate.astype(BF16), d_up.astype(BF16)))
            d_h_part = dot(d_gate, w_g, 1, 1) + dot(d_up, w_u, 1, 1)
            d_hs.append(lax.psum_scatter(d_h_part, PLANE, scatter_dimension=0, tiled=True).astype(BF16))
            y_part = dot(act_k, w_d, 1, 0)
            y_sums.append(plane_sum(y_part))
            hs.append(h_k)
            acts.append(act_k)
            d_gates.append(d_gate)
            d_ups.append(d_up)
        d_h_two = jnp.concatenate(d_hs)
        y_sum, resid_y = lax.optimization_barrier((jnp.concatenate(y_sums), resid_bf))
        layer_out = (resid_y.astype(F32) + y_sum).astype(BF16)
        h_all, d_gate, d_up = (jnp.concatenate(v) for v in (hs, d_gates, d_ups))
        act, dy_all = jnp.concatenate(acts), dys.reshape(-1, dim)

        def grad_xc(a, b, shape, c_dim):
            part = dot(a, b, 0, 0).reshape(shape)
            half = add_flip(part, c_i, c_dim, "c")
            return add_flip(half, x_i, c_dim - 1, "x").astype(BF16)

        def grad_all(a, b):
            part = dot(a, b, 0, 0).reshape(4, 2, 2, shard, -1)
            half = add_flip(part, c_i, 2, "c")
            half = lax.psum_scatter(half.reshape(8 * shard, -1), PLANE, scatter_dimension=0, tiled=True)
            return add_flip(half.reshape(2, shard, -1), x_i, 0, "x").astype(BF16)

        cols = (4, 2, 2, shard, ffn_q)
        g_gate = grad_xc(h_all, d_gate, cols, 2)
        g_up = grad_xc(h_all, d_up, cols, 2)
        g_down = grad_xc(act, dy_all, (2, 2, ffn // N_DEV, dim), 1)
        back = lax.all_to_all(jnp.stack([g_gate, g_up], axis=1), PLANE, 0, 0, tiled=True)
        back = back.transpose(1, 2, 0, 3).reshape(2, shard, ffn)

        d_resid_two, g_norm2 = norm2_pull(d_h_two)
        d_resid = (dy.astype(F32) + d_resid_two).astype(BF16)
        g_out = grad_all(o_bf, d_resid)
        d_attn = dot(d_resid, w_o, 1, 1).astype(BF16)
        d_query, d_key, d_value = attn_pull(d_attn[None])
        d_qkv = jnp.concatenate([d_query.astype(BF16).reshape(seq, -1), d_key.astype(BF16).reshape(seq, -1), d_value.reshape(seq, -1)], axis=1)
        g_qkv = grad_all(h_one, d_qkv)
        d_h_one = dot(d_qkv, w_qkv, 1, 1).astype(BF16)
        d_x, g_norm1 = norm1_pull(d_h_one)
        d_emb = (d_resid.astype(F32) + d_x).astype(BF16)

        d_slot = dot(pick, d_emb, 0, 0).reshape(N_DEV, SLOTS, dim)
        place = jnp.arange(SLOTS)[None, :, None]
        d_slot = jnp.where(place == USABLE, g_norm1, jnp.where(place == USABLE + 1, g_norm2, d_slot))
        d_got = lax.all_to_all(d_slot, ALL, 0, 0, tiled=True)
        gains = lax.dynamic_slice_in_dim(jnp.sum(d_got[:, USABLE:], axis=0), me * shard, shard, axis=1).astype(BF16)
        n_slot = N_DEV * SLOTS
        key = jnp.where(slot_used, slot_row, rows_dev).reshape(-1)
        key_sorted, order = lax.sort((key, jnp.arange(n_slot, dtype=jnp.int32)), num_keys=1)
        edges = jnp.minimum(jnp.arange(pl.cdiv(rows_dev, ROW_BLOCK) + 1) * ROW_BLOCK, rows_dev)
        starts = jnp.sum((key[None, :] < edges[:, None]).astype(jnp.int32), axis=1)

        def rows_dense():
            d_all = jnp.concatenate([d_emb] + [lax.ppermute(d_emb, ALL, ring(k)) for k in range(1, N_DEV)])
            origin = (me - jnp.arange(N_DEV)) % N_DEV
            seg = jnp.where(owner == me, rel, rows_dev)[origin].reshape(-1)
            return jax.ops.segment_sum(d_all.astype(F32), seg, num_segments=rows_dev).astype(BF16)

        d_rows = lax.cond(overflow, rows_dense, lambda: row_sums(starts, order, key_sorted, d_got.reshape(-1, dim), rows_dev))
        g_q = g_qkv[:, :q_w].reshape(w_query.shape)
        g_k = g_qkv[:, q_w : q_w + kv_w].reshape(w_key.shape)
        g_v = g_qkv[:, q_w + kv_w :].reshape(w_value.shape)
        return layer_out[None], d_rows, gains[0], gains[1], g_q, g_k, g_v, g_out, back[0], back[1], g_down

    return jax.shard_map(step, mesh=mesh, in_specs=in_specs, out_specs=out_specs, check_vma=False)
```
